32 devices in a mesh: tm: 8 (over z, y), freq: 4 (over x, core).
Axes of the slice: x: 2, y: 2, z: 4, core: 2. Of those that a mesh axis runs over, the one named last changes fastest.
Arguments:
- snapshots: bfloat16 [4352, 3, 4096], P('tm', None, 'freq'), may hold values from -200 to 200
- block_starts: int32 [32], replicated, may hold values from 0 to 4032, as said below
- freq_index: int32 [16], replicated, may hold values from 0 to 128
Outputs:
- modes: bfloat16 [16, 32, 2, 3, 4096], P(None, None, None, None, ('freq', 'tm'))
- energy: float32 [16], replicated
The draws below stay inside these ranges and needn't reach their ends.
Inputs may be any that keep to these rules, and one draw needn't show every extreme that they name: `block_starts`: block b starts at b * 128 plus between 0 and 64.
All inputs are finite; a program needn't handle non-finite values.
Results may differ from the reference program's by a relative error of at most 0.0085.
Values may be sent and summed in bfloat16 or wider, within the bound.
A program may use at most 64 MiB of HBM per device.

```python
import math
import jax
import jax.numpy as jnp
from jax import lax

NB = 32
NFFT = 256
NF = 16
HOP = 128
JIT = 64
TT = 4352
NSIT = 6
P_DEV = 128
P_SIZE = 4096


def draw_snapshots(key, part):
    key_noise, key_space, key_time = jax.random.split(key, 3)
    rising = jnp.exp(math.log(3.0) * jnp.arange(P_SIZE, dtype=jnp.float32) / P_SIZE)
    space_scale = rising * jnp.exp(jax.random.uniform(key_space, (P_SIZE,), minval=0.0, maxval=math.log(10.0))) / 3.0
    time_scale = jnp.exp(jax.random.uniform(key_time, (TT,), minval=math.log(0.3), maxval=math.log(3.0)))
    values = jnp.clip(jax.random.normal(key_noise, (TT, 3, P_SIZE)), -5.0, 5.0)
    return (values * time_scale[:, None, None] * space_scale[None, None, :]).astype(jnp.bfloat16)


def draw_block_starts(key, part):
    jitter = jax.random.randint(key, (NB,), 0, JIT + 1)
    return (jnp.arange(NB, dtype=jnp.int32) * HOP + jitter).astype(jnp.int32)


def set_ends(drawn, rng, low, top_value):
    dims = drawn.shape
    index_at = [jax.random.randint(jax.random.fold_in(rng, axis), (), 0, dims[axis]) for axis in range(len(dims))]
    drawn = drawn.at[tuple(index_at)].set(low)
    longest = dims.index(max(dims))
    index_at[longest] = (index_at[longest] + 1) % dims[longest]
    return drawn.at[tuple(index_at)].set(top_value)


def setup_inputs(seed: int = 0) -> dict:
    key_list = jax.random.split(jax.random.key(seed), 4)
    return {
        "snapshots": draw_snapshots(jax.random.fold_in(key_list[3], 71), 0),
        "block_starts": draw_block_starts(jax.random.fold_in(key_list[3], 71), 0),
        "freq_index": set_ends(jax.random.randint(key_list[2], (NF,), 0, NFFT // 2 + 1), jax.random.fold_in(key_list[2], 1), 0, (NFFT // 2 + 1) - 1).astype(jnp.int32),
    }


def dft_rows(freq_index):
    times_idx = jnp.arange(NFFT, dtype=jnp.int32)
    phase_int = freq_index[:, None].astype(jnp.int32) * times_idx[None, :] % NFFT
    angles = 2.0 * math.pi / NFFT * phase_int.astype(jnp.float32)
    window = 0.5 - 0.5 * jnp.cos(2.0 * math.pi / NFFT * times_idx.astype(jnp.float32))
    scaling = 1.0 / jnp.sqrt(jnp.sum(window * window))
    cosine = window[None, :] * jnp.cos(angles) * scaling
    sine_rows = -window[None, :] * jnp.sin(angles) * scaling
    return jnp.stack([cosine, sine_rows], 1).reshape(2 * NF, NFFT).astype(jnp.bfloat16)

def block_rows(block_starts):
    return block_starts[:, None].astype(jnp.int32) + jnp.arange(NFFT, dtype=jnp.int32)[None, :]

def matmul_batch(left, right):
    return jnp.einsum('fij,fjk->fik', left, right, precision=lax.Precision.HIGHEST)

def whiten(summed, points):
    gram_re = summed[:, 0]
    gram_im = summed[:, 1]
    top_rows = jnp.concatenate([gram_re, -gram_im], 2)
    low_rows = jnp.concatenate([gram_im, gram_re], 2)
    hermit = jnp.concatenate([top_rows, low_rows], 1)
    frob = jnp.sqrt(lax.optimization_barrier(jnp.sum(hermit * hermit, axis=(1, 2))) + 1e-06)
    identity = jnp.eye(2 * NB, dtype=jnp.float32)[None]
    iterate = hermit / frob[:, None, None]
    inverse = jnp.broadcast_to(identity, hermit.shape)
    for iteration in range(NSIT):
        factor = 1.5 * identity - 0.5 * matmul_batch(inverse, iterate)
        iterate = matmul_batch(iterate, factor)
        inverse = matmul_batch(factor, inverse)
    columns = inverse[:, :, :NB] * jnp.sqrt(6.0 * points / frob)[:, None, None]
    upper = columns[:, :NB]
    lower = columns[:, NB:]
    coefficients = jnp.stack([jnp.stack([upper, -lower], 1), jnp.stack([lower, upper], 1)], 1)
    energy = jnp.trace(gram_re, axis1=1, axis2=2) / (3.0 * NB * points)
    return (coefficients, energy)

def reference(snapshots, block_starts, freq_index):
    dft_table = dft_rows(freq_index).astype(jnp.float32)
    offsets = block_rows(block_starts)
    columns_all = snapshots.reshape(TT, 3 * P_SIZE)
    block_cols = 16 * P_DEV

    def spectra_block(start):
        piece = lax.dynamic_slice_in_dim(columns_all, start, block_cols, 1)
        windows = jnp.take(piece, offsets, axis=0).astype(jnp.float32)
        return jnp.einsum('rt,btn->brn', dft_table, windows, precision=lax.Precision.HIGHEST).astype(jnp.bfloat16)
    starts = jnp.arange(3 * P_SIZE // block_cols, dtype=jnp.int32) * block_cols
    pieces = lax.map(spectra_block, starts)
    spectra = jnp.transpose(pieces, (1, 2, 0, 3)).reshape(NB, NF, 2, 3 * P_SIZE)
    by_freq = jnp.moveaxis(spectra, 1, 0)

    def gram_one(spec_f):
        real_part = spec_f[:, 0].astype(jnp.float32)
        imag_part = spec_f[:, 1].astype(jnp.float32)
        gram_re = jnp.dot(real_part, real_part.T, precision=lax.Precision.HIGHEST) + jnp.dot(imag_part, imag_part.T, precision=lax.Precision.HIGHEST)
        cross_terms = jnp.dot(real_part, imag_part.T, precision=lax.Precision.HIGHEST)
        return jnp.stack([gram_re, cross_terms - cross_terms.T])
    summed = lax.map(gram_one, by_freq)
    coefficients, energy = whiten(summed, float(P_SIZE))
    coef_bf = coefficients.astype(jnp.bfloat16)

    def modes_one(pair):
        coef_f, spec_f = pair
        return jnp.einsum('orbj,brn->jon', coef_f.astype(jnp.float32), spec_f.astype(jnp.float32), precision=lax.Precision.HIGHEST).astype(jnp.bfloat16)
    modes = lax.map(modes_one, (coef_bf, by_freq))
    return (modes.reshape(NF, NB, 2, 3, P_SIZE), energy)
```

```python
import functools
import math

import jax
import jax.numpy as jnp
from jax import lax
from jax.experimental import pallas as pl
from jax.experimental.pallas import tpu as pltpu
from jax.sharding import PartitionSpec as P

NB = 32
NFFT = 256
NF = 16
NSIT = 6


def for_sending(shard):
    return jax.tree.map(lambda a: a.astype(jnp.bfloat16) if a.dtype == jnp.float32 else a, shard)


def dft_rows(freq_index):
    times_idx = jnp.arange(NFFT, dtype=jnp.int32)
    phase_int = freq_index[:, None] * times_idx[None, :] % NFFT
    angles = 2.0 * math.pi / NFFT * phase_int.astype(jnp.float32)
    window = 0.5 - 0.5 * jnp.cos(2.0 * math.pi / NFFT * times_idx.astype(jnp.float32))
    scaling = 1.0 / jnp.sqrt(jnp.sum(window * window))
    cosine = window[None, :] * jnp.cos(angles) * scaling
    sine_rows = -window[None, :] * jnp.sin(angles) * scaling
    return jnp.stack([cosine, sine_rows], 1).reshape(2 * NF, NFFT).astype(jnp.bfloat16)


def block_rows(block_starts):
    return block_starts[:, None] + jnp.arange(NFFT, dtype=jnp.int32)[None, :]


def matmul_batch(left, right):
    return jnp.einsum("fij,fjk->fik", left, right, precision=lax.Precision.HIGHEST)


def whiten(summed, points):
    gram_re = summed[:, 0]
    gram_im = summed[:, 1]
    top_rows = jnp.concatenate([gram_re, -gram_im], 2)
    low_rows = jnp.concatenate([gram_im, gram_re], 2)
    hermit = jnp.concatenate([top_rows, low_rows], 1)
    frob = jnp.sqrt(jnp.sum(hermit * hermit, axis=(1, 2)) + 1e-06)
    identity = jnp.eye(2 * NB, dtype=jnp.float32)[None]
    iterate = hermit / frob[:, None, None]
    inverse = jnp.broadcast_to(identity, hermit.shape)
    for iteration in range(NSIT):
        factor = 1.5 * identity - 0.5 * matmul_batch(inverse, iterate)
        iterate = matmul_batch(iterate, factor)
        inverse = matmul_batch(factor, inverse)
    columns = inverse[:, :, :NB] * jnp.sqrt(6.0 * points / frob)[:, None, None]
    upper = columns[:, :NB]
    lower = columns[:, NB:]
    coefficients = jnp.stack([jnp.stack([upper, -lower], 1), jnp.stack([lower, upper], 1)], 1)
    energy = jnp.trace(gram_re, axis1=1, axis2=2) / (3.0 * NB * points)
    return (coefficients, energy)


def local(snapshots, block_starts, freq_index):
    dft_table = dft_rows(freq_index)
    offsets = block_rows(block_starts)
    series = lax.all_to_all(snapshots, "tm", split_axis=2, concat_axis=0, tiled=True)
    count = series.shape[1]
    width = series.shape[2]
    columns_all = series.reshape(series.shape[0], count * width)
    windows = jnp.take(columns_all, offsets, axis=0)
    spectra_part = jnp.einsum(
        "rt,btn->rbn", dft_table, windows, preferred_element_type=jnp.float32
    ).astype(jnp.bfloat16)
    spectra = spectra_part.reshape(2 * NF, NB, count, width)
    width = spectra.shape[3]
    points = float(width * lax.axis_size("tm") * lax.axis_size("freq"))
    flat_spec = spectra.reshape(NF, 2, NB, 3 * width)
    real_part = flat_spec[:, 0]
    imag_part = flat_spec[:, 1]
    gram_re = jnp.einsum("fbn,fcn->fbc", real_part, real_part, preferred_element_type=jnp.float32)
    gram_re = gram_re + jnp.einsum(
        "fbn,fcn->fbc", imag_part, imag_part, preferred_element_type=jnp.float32
    )
    cross_terms = jnp.einsum(
        "fbn,fcn->fbc", real_part, imag_part, preferred_element_type=jnp.float32
    )
    partial_gram = jnp.stack([gram_re, cross_terms - jnp.swapaxes(cross_terms, 1, 2)], 1)
    shared = lax.psum_scatter(partial_gram, "freq", scatter_dimension=0, tiled=True)
    shared = lax.psum(shared, "tm")
    coef_part, energy_part = whiten(shared, points)
    coefficients, energy = (
        lax.all_gather(for_sending(coef_part), "freq", axis=0, tiled=True).astype(coef_part.dtype),
        lax.all_gather(for_sending(energy_part), "freq", axis=0, tiled=True).astype(
            energy_part.dtype
        ),
    )
    coef_bf = jnp.transpose(coefficients.astype(jnp.bfloat16), (0, 4, 1, 2, 3))
    modes = jnp.einsum(
        "fjorb,frbn->fjon", coef_bf, flat_spec, preferred_element_type=jnp.float32
    ).astype(jnp.bfloat16)
    return (modes.reshape(NF, NB, 2, 3, width), energy)


MESH = pl.DeviceIdType.MESH
ROWS = 2 * NF
HOP = 128
JIT = 64


def plan(n, rows, total, width):
    if n < 2 or NB % n or total % NF or total // NF < 1 or width != 128 or rows % 16:
        return None
    per = NB // n
    if per < 4:
        return None
    left, right = [[], []], [[], []]
    for dev in range(n):
        first, end = rows * dev, rows * (dev + 1)
        for block in range(NB):
            if HOP * block >= end or HOP * block + JIT + NFFT <= first:
                continue
            owner = block // per
            if owner == dev:
                continue
            if owner == dev - 1 and per * dev - block <= 2:
                left[per * dev - block - 1].append(dev)
            elif owner == dev + 1 and block - per * (dev + 1) < 2:
                right[block - per * (dev + 1)].append(dev)
            else:
                return None
    for devs in left + right:
        if devs and devs != list(range(devs[0], devs[-1] + 1)):
            return None
    return per, left, right


def shifted_tables(block_starts, freq_index, n, per, rows):
    me = lax.axis_index("tm")
    offsets = jnp.array([-1, -2, per, per + 1] + list(range(per)), dtype=jnp.int32)
    ids = per * me + offsets
    starts = jnp.take(block_starts, jnp.clip(ids, 0, NB - 1))
    local_t = rows * me + jnp.arange(rows, dtype=jnp.int32)[None, :] - starts[:, None]
    inside = (local_t >= 0) & (local_t < NFFT) & ((ids >= 0) & (ids < NB))[:, None]
    local_t = jnp.where(inside, local_t, 0)
    times_idx = jnp.arange(NFFT, dtype=jnp.int32)
    full_window = 0.5 - 0.5 * jnp.cos(2.0 * math.pi / NFFT * times_idx.astype(jnp.float32))
    scaling = 1.0 / jnp.sqrt(jnp.sum(full_window * full_window))
    window = 0.5 - 0.5 * jnp.cos(2.0 * math.pi / NFFT * local_t.astype(jnp.float32))
    window = jnp.where(inside, window, 0.0)
    freqs = jnp.repeat(freq_index, 2)
    phase = freqs[None, :, None] * local_t[:, None, :] % NFFT
    angles = 2.0 * math.pi / NFFT * phase.astype(jnp.float32)
    is_sine = (jnp.arange(ROWS) % 2 == 1)[None, :, None]
    wave = jnp.where(is_sine, -jnp.sin(angles), jnp.cos(angles))
    table = window[:, None, :] * wave * scaling
    return table.reshape((per + 4) * ROWS, rows).astype(jnp.bfloat16)


def expanders():
    row = jnp.arange(NB * 6)
    col = jnp.arange(2 * NB)
    spread = (row[:, None] // 6 == col[None, :] % NB) & (row[:, None] % 2 == col[None, :] // NB)
    wide = jnp.arange(3 * 2 * NB)
    mask = row[:, None] // 2 % 3 == wide[None, :] // (2 * NB)
    return spread.astype(jnp.bfloat16), mask.astype(jnp.float32)


def within(me, devs):
    return (me >= devs[0]) & (me <= devs[-1])


def kernel(n, nf_dev, per, left, right, points, x_hbm, t_ref, spread_ref, mask_ref,
           modes_ref, energy_ref, xv, out_l, out_r, in_l, in_r, own, sendb, recvb, spec32, spec,
           gpart, gath, msg, crecv, load_sem, lsend, lrecv, rsend, rrecv, asend, arecv,
           gsend, grecv, csend, crcv):
    tm = lax.axis_index("tm")
    fr = lax.axis_index("freq")
    total = n * nf_dev
    lin = tm * nf_dev + fr
    stride = total // NF

    def where_is(index):
        return {"tm": index // nf_dev, "freq": index % nf_dev}

    for c in range(3):
        pltpu.make_async_copy(x_hbm.at[c], xv.at[c], load_sem.at[c]).start()
    barrier = pltpu.get_barrier_semaphore()

    @pl.loop(1, total)
    def _(k):
        pl.semaphore_signal(barrier, inc=1, device_id=where_is((lin + k) % total), device_id_type=MESH)

    width = xv.shape[2]
    for c in range(3):
        pltpu.make_async_copy(x_hbm.at[c], xv.at[c], load_sem.at[c]).wait()
        part = jnp.dot(t_ref[: 4 * ROWS, :], xv[c], preferred_element_type=jnp.float32)
        for slot in range(2):
            out_l[slot, :, c * width : (c + 1) * width] = part[slot * ROWS : (slot + 1) * ROWS]
            out_r[slot, :, c * width : (c + 1) * width] = part[(slot + 2) * ROWS : (slot + 3) * ROWS]
    pl.semaphore_wait(barrier, total - 1)

    def to_left(slot):
        return pltpu.make_async_remote_copy(
            src_ref=out_l.at[slot], dst_ref=in_r.at[slot], send_sem=lsend.at[slot],
            recv_sem=lrecv.at[slot], device_id={"tm": (tm + n - 1) % n, "freq": fr},
            device_id_type=MESH)

    def to_right(slot):
        return pltpu.make_async_remote_copy(
            src_ref=out_r.at[slot], dst_ref=in_l.at[slot], send_sem=rsend.at[slot],
            recv_sem=rrecv.at[slot], device_id={"tm": (tm + 1) % n, "freq": fr},
            device_id_type=MESH)

    for slot in range(2):
        for devs, make in ((left[slot], to_left), (right[slot], to_right)):
            if devs:
                @pl.when(within(tm, devs))
                def _(make=make, slot=slot):
                    make(slot).start()

    for c in range(3):
        own[:, c * width : (c + 1) * width] = jnp.dot(
            t_ref[4 * ROWS :, :], xv[c], preferred_element_type=jnp.float32)

    def scatter(block, k):
        dest = (tm + k) % n
        return pltpu.make_async_remote_copy(
            src_ref=sendb.at[dest, block], dst_ref=recvb.at[tm, block],
            send_sem=asend.at[block, dest], recv_sem=arecv.at[block, tm],
            device_id={"tm": dest, "freq": fr}, device_id_type=MESH)

    order = list(range(2, per - 2)) + [1, per - 2, per - 1, 0]
    for block in order:
        span = slice(block * ROWS, (block + 1) * ROWS)
        if block < 2 and right[block]:
            @pl.when(within(tm - 1, right[block]))
            def _(block=block, span=span):
                to_right(block).wait_recv()
                own[span, :] += in_l[block]
        back = per - 1 - block
        if back < 2 and left[back]:
            @pl.when(within(tm + 1, left[back]))
            def _(back=back, span=span):
                to_left(back).wait_recv()
                own[span, :] += in_r[back]
        pw = width // n
        for dest in range(n):
            for c in range(3):
                sendb[dest, block, :, c * pw : (c + 1) * pw] = own[
                    span, c * width + dest * pw : c * width + (dest + 1) * pw].astype(jnp.bfloat16)

        @pl.loop(1, n)
        def _(k, block=block):
            scatter(block, k).start()

    def widen(src, block, values):
        base = (src * per + block) * ROWS
        for c in range(3):
            spec32[c, pl.ds(pl.multiple_of(base, ROWS), ROWS), :] = values[:, c * 128 : (c + 1) * 128].astype(jnp.float32)

    for block in range(per):
        widen(tm, block, sendb[tm, block])

    @pl.loop(1, n)
    def _(k):
        src = (tm + n - k) % n
        for block in range(per):
            pltpu.make_async_remote_copy(
                src_ref=sendb.at[src, block], dst_ref=recvb.at[src, block],
                send_sem=asend.at[block, src], recv_sem=arecv.at[block, src],
                device_id={"tm": src, "freq": fr}, device_id_type=MESH).wait_recv()
            widen(src, block, recvb[src, block])

    def to_owner(f):
        return pltpu.make_async_remote_copy(
            src_ref=gpart.at[f], dst_ref=gath.at[lin], send_sem=gsend.at[f],
            recv_sem=grecv.at[lin], device_id=where_is(f * stride), device_id_type=MESH)

    for f in range(NF):
        real = [spec32[c, pl.ds(2 * f, NB, stride=ROWS), :].astype(jnp.bfloat16) for c in range(3)]
        imag = [spec32[c, pl.ds(2 * f + 1, NB, stride=ROWS), :].astype(jnp.bfloat16) for c in range(3)]
        for c in range(3):
            spec[f, c * 2 * NB : c * 2 * NB + NB, :] = real[c]
            spec[f, c * 2 * NB + NB : (c + 1) * 2 * NB, :] = imag[c]
        lhs = jnp.concatenate(real + imag, axis=1)
        rhs = jnp.concatenate([lhs, jnp.concatenate(imag + [-v for v in real], axis=1)], axis=0)
        gram = lax.dot_general(lhs, rhs, (((1,), (1,)), ((), ())), preferred_element_type=jnp.float32)
        half = NB // 2
        gpart[f] = jnp.concatenate([gram[:half], gram[half:]], axis=1)

        @pl.when(lin != f * stride)
        def _(f=f):
            to_owner(f).start()

    def coef_to(index):
        return pltpu.make_async_remote_copy(
            src_ref=msg, dst_ref=crecv.at[lin // stride], send_sem=csend.at[index],
            recv_sem=crcv.at[lin // stride], device_id=where_is(index), device_id_type=MESH)

    @pl.when(lin % stride == 0)
    def _():
        f_mine = lin // stride
        gath[lin] = gpart[f_mine]

        @pl.loop(1, total)
        def _(k):
            src = (lin + k) % total
            pltpu.make_async_remote_copy(
                src_ref=gpart.at[0], dst_ref=gath.at[src], send_sem=gsend.at[0],
                recv_sem=grecv.at[src], device_id=where_is(src), device_id_type=MESH).wait_recv()

        packed = jnp.sum(gath[...], axis=0)
        both = jnp.concatenate([packed[:, : 2 * NB], packed[:, 2 * NB :]], axis=0)
        gram_re = both[:, :NB]
        gram_im = both[:, NB:]
        hermit = jnp.concatenate([
            jnp.concatenate([gram_re, -gram_im], axis=1),
            jnp.concatenate([gram_im, gram_re], axis=1)], axis=0)
        frob = jnp.sqrt(jnp.sum(hermit * hermit, axis=(0, 1), keepdims=True) + 1e-06)
        ri = lax.broadcasted_iota(jnp.int32, (2 * NB, 2 * NB), 0)
        ci = lax.broadcasted_iota(jnp.int32, (2 * NB, 2 * NB), 1)
        identity = jnp.where(ri == ci, 1.0, 0.0).astype(jnp.float32)
        energy = jnp.sum(jnp.where((ri == ci) & (ri < NB), hermit, 0.0), axis=(0, 1), keepdims=True) / (3.0 * NB * points)

        def mul(a, b):
            return jnp.dot(a, b, precision=lax.Precision.HIGHEST, preferred_element_type=jnp.float32)

        iterate = hermit / frob
        inverse = identity
        for step in range(NSIT):
            factor = 1.5 * identity - 0.5 * (iterate if step == 0 else mul(inverse, iterate))
            if step < NSIT - 1:
                iterate = mul(iterate, factor)
                inverse = factor if step == 0 else mul(factor, inverse)
            else:
                inverse = mul(factor[:NB], inverse)
        scaled = inverse[:NB] * jnp.sqrt(6.0 * points / frob)
        upper = scaled[:, :NB]
        lower = scaled[:, NB:]
        msg[:NB, :] = jnp.concatenate([upper, -lower, lower, upper], axis=1).astype(jnp.bfloat16)
        high = energy.astype(jnp.bfloat16).astype(jnp.float32)
        lane = lax.broadcasted_iota(jnp.int32, (16, 128), 1)
        tail = jnp.where(lane == 0, high, jnp.where(lane == 1, energy - high, 0.0))
        msg[NB:, :] = tail.astype(jnp.bfloat16)
        crecv[f_mine] = msg[...]

        @pl.loop(1, total)
        def _(k):
            coef_to((lin + k) % total).start()

    for f in range(NF):
        @pl.when(lin != f * stride)
        def _(f=f):
            pltpu.make_async_remote_copy(
                src_ref=msg, dst_ref=crecv.at[f], send_sem=csend.at[f], recv_sem=crcv.at[f],
                device_id=where_is(f * stride), device_id_type=MESH).wait_recv()

        pairs = crecv[f, :NB, :]
        stacked = jnp.concatenate([pairs[:, : 2 * NB], pairs[:, 2 * NB :]], axis=0)
        tiled = jnp.concatenate([stacked] * 3, axis=1)
        full = jnp.dot(spread_ref[...], tiled, preferred_element_type=jnp.float32)
        full = (full * mask_ref[...]).astype(jnp.bfloat16)
        modes_ref[f * 6 * NB : (f + 1) * 6 * NB, :] = jnp.dot(
            full, spec[f], preferred_element_type=jnp.float32).astype(jnp.bfloat16)
        tail = crecv[f, NB:, :].astype(jnp.float32)
        energy_ref[f : f + 1, :] = jnp.broadcast_to(jnp.sum(tail[:1, :], axis=1, keepdims=True), (1, 128))

    for slot in range(2):
        for devs, make in ((left[slot], to_left), (right[slot], to_right)):
            if devs:
                @pl.when(within(tm, devs))
                def _(make=make, slot=slot):
                    make(slot).wait_send()

    @pl.loop(1, n)
    def _(k):
        for block in range(per):
            scatter(block, k).wait_send()

    for f in range(NF):
        @pl.when(lin != f * stride)
        def _(f=f):
            to_owner(f).wait_send()

    @pl.when(lin % stride == 0)
    def _():
        @pl.loop(1, total)
        def _(k):
            coef_to((lin + k) % total).wait_send()


def fused(n, nf_dev, chosen, snapshots, block_starts, freq_index):
    per, left, right = chosen
    rows, count, wide = snapshots.shape
    total = n * nf_dev
    tables = shifted_tables(block_starts, freq_index, n, per, rows)
    spread, mask = expanders()
    pw = wide // n
    f32, bf16 = jnp.float32, jnp.bfloat16
    dma = pltpu.SemaphoreType.DMA
    vmem = pl.BlockSpec(memory_space=pltpu.VMEM)
    modes, energy = pl.pallas_call(
        functools.partial(kernel, n, nf_dev, per, left, right, float(wide * nf_dev)),
        out_shape=(jax.ShapeDtypeStruct((NF * NB * 6, pw), bf16), jax.ShapeDtypeStruct((NF, 128), f32)),
        in_specs=[pl.BlockSpec(memory_space=pl.ANY), vmem, vmem, vmem],
        out_specs=(vmem, vmem),
        scratch_shapes=[
            pltpu.VMEM((3, rows, wide), bf16),
            pltpu.VMEM((2, ROWS, 3 * wide), f32),
            pltpu.VMEM((2, ROWS, 3 * wide), f32),
            pltpu.VMEM((2, ROWS, 3 * wide), f32),
            pltpu.VMEM((2, ROWS, 3 * wide), f32),
            pltpu.VMEM((per * ROWS, 3 * wide), f32),
            pltpu.VMEM((n, per, ROWS, 3 * pw), bf16),
            pltpu.VMEM((n, per, ROWS, 3 * pw), bf16),
            pltpu.VMEM((3, NB * ROWS, pw), f32),
            pltpu.VMEM((NF, 6 * NB, pw), bf16),
            pltpu.VMEM((NF, NB // 2, 4 * NB), f32),
            pltpu.VMEM((total, NB // 2, 4 * NB), f32),
            pltpu.VMEM((NB + 16, 4 * NB), bf16),
            pltpu.VMEM((NF, NB + 16, 4 * NB), bf16),
            dma((3,)), dma((2,)), dma((2,)), dma((2,)), dma((2,)),
            dma((per, n)), dma((per, n)), dma((NF,)), dma((total,)), dma((total,)), dma((NF,)),
        ],
        compiler_params=pltpu.CompilerParams(
            collective_id=0, has_side_effects=True, vmem_limit_bytes=48 * 1024 * 1024),
    )(jnp.transpose(snapshots, (1, 0, 2)), tables, spread, mask)
    modes = modes.reshape(NF, NB, 3, 2, pw).transpose(0, 1, 3, 2, 4)
    return modes, energy[:, 0]


def solution(mesh):
    n, nf_dev = mesh.shape["tm"], mesh.shape["freq"]

    def body(snapshots, block_starts, freq_index):
        rows, _, wide = snapshots.shape
        chosen = plan(n, rows, n * nf_dev, wide // n)
        if chosen is None:
            return local(snapshots, block_starts, freq_index)
        return fused(n, nf_dev, chosen, snapshots, block_starts, freq_index)

    return jax.shard_map(
        body,
        mesh=mesh,
        in_specs=(P("tm", None, "freq"), P(), P()),
        out_specs=(P(None, None, None, None, ("freq", "tm")), P()),
        check_vma=False,
    )
```

```python
import functools
import math

import jax
import jax.numpy as jnp
import numpy as np
from jax import lax
from jax.experimental import pallas as pl
from jax.experimental.pallas import tpu as pltpu
from jax.sharding import PartitionSpec as P

NB = 32
NFFT = 256
NF = 16
NSIT = 6


def for_sending(shard):
    return jax.tree.map(lambda a: a.astype(jnp.bfloat16) if a.dtype == jnp.float32 else a, shard)


def dft_rows(freq_index):
    times_idx = jnp.arange(NFFT, dtype=jnp.int32)
    phase_int = freq_index[:, None] * times_idx[None, :] % NFFT
    angles = 2.0 * math.pi / NFFT * phase_int.astype(jnp.float32)
    window = 0.5 - 0.5 * jnp.cos(2.0 * math.pi / NFFT * times_idx.astype(jnp.float32))
    scaling = 1.0 / jnp.sqrt(jnp.sum(window * window))
    cosine = window[None, :] * jnp.cos(angles) * scaling
    sine_rows = -window[None, :] * jnp.sin(angles) * scaling
    return jnp.stack([cosine, sine_rows], 1).reshape(2 * NF, NFFT).astype(jnp.bfloat16)


def block_rows(block_starts):
    return block_starts[:, None] + jnp.arange(NFFT, dtype=jnp.int32)[None, :]


def matmul_batch(left, right):
    return jnp.einsum("fij,fjk->fik", left, right, precision=lax.Precision.HIGHEST)


def whiten(summed, points):
    gram_re = summed[:, 0]
    gram_im = summed[:, 1]
    top_rows = jnp.concatenate([gram_re, -gram_im], 2)
    low_rows = jnp.concatenate([gram_im, gram_re], 2)
    hermit = jnp.concatenate([top_rows, low_rows], 1)
    frob = jnp.sqrt(jnp.sum(hermit * hermit, axis=(1, 2)) + 1e-06)
    identity = jnp.eye(2 * NB, dtype=jnp.float32)[None]
    iterate = hermit / frob[:, None, None]
    inverse = jnp.broadcast_to(identity, hermit.shape)
    for iteration in range(NSIT):
        factor = 1.5 * identity - 0.5 * matmul_batch(inverse, iterate)
        iterate = matmul_batch(iterate, factor)
        inverse = matmul_batch(factor, inverse)
    columns = inverse[:, :, :NB] * jnp.sqrt(6.0 * points / frob)[:, None, None]
    upper = columns[:, :NB]
    lower = columns[:, NB:]
    coefficients = jnp.stack([jnp.stack([upper, -lower], 1), jnp.stack([lower, upper], 1)], 1)
    energy = jnp.trace(gram_re, axis1=1, axis2=2) / (3.0 * NB * points)
    return (coefficients, energy)


def local(snapshots, block_starts, freq_index):
    dft_table = dft_rows(freq_index)
    offsets = block_rows(block_starts)
    series = lax.all_to_all(snapshots, "tm", split_axis=2, concat_axis=0, tiled=True)
    count = series.shape[1]
    width = series.shape[2]
    columns_all = series.reshape(series.shape[0], count * width)
    windows = jnp.take(columns_all, offsets, axis=0)
    spectra_part = jnp.einsum(
        "rt,btn->rbn", dft_table, windows, preferred_element_type=jnp.float32
    ).astype(jnp.bfloat16)
    spectra = spectra_part.reshape(2 * NF, NB, count, width)
    width = spectra.shape[3]
    points = float(width * lax.axis_size("tm") * lax.axis_size("freq"))
    flat_spec = spectra.reshape(NF, 2, NB, 3 * width)
    real_part = flat_spec[:, 0]
    imag_part = flat_spec[:, 1]
    gram_re = jnp.einsum("fbn,fcn->fbc", real_part, real_part, preferred_element_type=jnp.float32)
    gram_re = gram_re + jnp.einsum(
        "fbn,fcn->fbc", imag_part, imag_part, preferred_element_type=jnp.float32
    )
    cross_terms = jnp.einsum(
        "fbn,fcn->fbc", real_part, imag_part, preferred_element_type=jnp.float32
    )
    partial_gram = jnp.stack([gram_re, cross_terms - jnp.swapaxes(cross_terms, 1, 2)], 1)
    shared = lax.psum_scatter(partial_gram, "freq", scatter_dimension=0, tiled=True)
    shared = lax.psum(shared, "tm")
    coef_part, energy_part = whiten(shared, points)
    coefficients, energy = (
        lax.all_gather(for_sending(coef_part), "freq", axis=0, tiled=True).astype(coef_part.dtype),
        lax.all_gather(for_sending(energy_part), "freq", axis=0, tiled=True).astype(
            energy_part.dtype
        ),
    )
    coef_bf = jnp.transpose(coefficients.astype(jnp.bfloat16), (0, 4, 1, 2, 3))
    modes = jnp.einsum(
        "fjorb,frbn->fjon", coef_bf, flat_spec, preferred_element_type=jnp.float32
    ).astype(jnp.bfloat16)
    return (modes.reshape(NF, NB, 2, 3, width), energy)


MESH = pl.DeviceIdType.MESH
ROWS = 2 * NF
HOP = 128
JIT = 64


def plan(n, rows, total, width):
    if n < 2 or NB % n or total % NF or total // NF < 1 or width != 128 or rows % 16:
        return None
    per = NB // n
    if per < 4:
        return None
    left, right = [[], []], [[], []]
    for dev in range(n):
        first, end = rows * dev, rows * (dev + 1)
        for block in range(NB):
            if HOP * block >= end or HOP * block + JIT + NFFT <= first:
                continue
            owner = block // per
            if owner == dev:
                continue
            if owner == dev - 1 and per * dev - block <= 2:
                left[per * dev - block - 1].append(dev)
            elif owner == dev + 1 and block - per * (dev + 1) < 2:
                right[block - per * (dev + 1)].append(dev)
            else:
                return None
    for devs in left + right:
        if devs and devs != list(range(devs[0], devs[-1] + 1)):
            return None
    return per, left, right


def base_table(freq_ref):
    row = lax.broadcasted_iota(jnp.int32, (ROWS, NFFT), 0)
    times_idx = lax.broadcasted_iota(jnp.int32, (ROWS, NFFT), 1)
    freqs = jnp.zeros((ROWS, NFFT), jnp.int32)
    for f in range(NF):
        freqs = jnp.where((row >> 1) == f, freq_ref[f], freqs)
    phase = (freqs * times_idx) & (NFFT - 1)
    angles = 2.0 * math.pi / NFFT * phase.astype(jnp.float32)
    window = 0.5 - 0.5 * jnp.cos(2.0 * math.pi / NFFT * times_idx.astype(jnp.float32))
    hann = 0.5 - 0.5 * np.cos(2.0 * math.pi / NFFT * np.arange(NFFT))
    scaling = np.float32(1.0 / np.sqrt(np.sum(hann * hann)))
    cosine = window * jnp.cos(angles) * scaling
    sine = -window * jnp.sin(angles) * scaling
    return jnp.where((row & 1) == 1, sine, cosine).astype(jnp.bfloat16)


def shifted(base, shift, rows):
    source = lax.broadcasted_iota(jnp.int32, (NFFT, rows), 0)
    target = lax.broadcasted_iota(jnp.int32, (NFFT, rows), 1)
    pick = jnp.where(source - target == shift, 1.0, 0.0).astype(jnp.bfloat16)
    return jnp.dot(base, pick, preferred_element_type=jnp.float32).astype(jnp.bfloat16)


def expanders(spread_ref, mask_ref):
    row = lax.broadcasted_iota(jnp.int32, (NB * 6, 2 * NB), 0)
    col = lax.broadcasted_iota(jnp.int32, (NB * 6, 2 * NB), 1)
    first = 6 * (col & (NB - 1))
    hit = (row >= first) & (row < first + 6) & ((row & 1) == jnp.where(col >= NB, 1, 0))
    spread_ref[...] = jnp.where(hit, 1.0, 0.0).astype(jnp.bfloat16)
    row = lax.broadcasted_iota(jnp.int32, (NB * 6, 6 * NB), 0)
    col = lax.broadcasted_iota(jnp.int32, (NB * 6, 6 * NB), 1)
    pair = row >> 1
    comp = pair - 3 * ((pair * 43691) >> 17)
    part = jnp.where(col >= 4 * NB, 2, jnp.where(col >= 2 * NB, 1, 0))
    mask_ref[...] = jnp.where(comp == part, 1.0, 0.0)


def within(me, devs):
    return (me >= devs[0]) & (me <= devs[-1])


def kernel(n, nf_dev, per, left, right, points, x_hbm, starts_ref, freq_ref,
           modes_ref, energy_ref, t_ref, spread_ref, mask_ref, xv, out_l, out_r, in_l, in_r, own, sendb, recvb, spec32, spec,
           gpart, gath, msg, crecv, load_sem, lsend, lrecv, rsend, rrecv, asend, arecv,
           gsend, grecv, csend, crcv):
    tm = lax.axis_index("tm")
    fr = lax.axis_index("freq")
    total = n * nf_dev
    lin = tm * nf_dev + fr
    stride = total // NF

    def where_is(index):
        return {"tm": index // nf_dev, "freq": index % nf_dev}

    for c in range(3):
        pltpu.make_async_copy(x_hbm.at[c], xv.at[c], load_sem.at[c]).start()
    barrier = pltpu.get_barrier_semaphore()

    @pl.loop(1, total)
    def _(k):
        pl.semaphore_signal(barrier, inc=1, device_id=where_is((lin + k) % total), device_id_type=MESH)

    rows = xv.shape[1]
    base = base_table(freq_ref)
    for slot, offset in enumerate([-1, -2, per, per + 1] + list(range(per))):
        block = per * tm + offset
        start = starts_ref[jnp.clip(block, 0, NB - 1)]
        inside = (block >= 0) & (block < NB)
        shift = jnp.where(inside, rows * tm - start, 4 * (rows + NFFT))
        t_ref[slot * ROWS : (slot + 1) * ROWS, :] = shifted(base, shift, rows)
    expanders(spread_ref, mask_ref)
    width = xv.shape[2]
    for c in range(3):
        pltpu.make_async_copy(x_hbm.at[c], xv.at[c], load_sem.at[c]).wait()
        part = jnp.dot(t_ref[: 4 * ROWS, :], xv[c], preferred_element_type=jnp.float32)
        for slot in range(2):
            out_l[slot, :, c * width : (c + 1) * width] = part[slot * ROWS : (slot + 1) * ROWS]
            out_r[slot, :, c * width : (c + 1) * width] = part[(slot + 2) * ROWS : (slot + 3) * ROWS]
    pl.semaphore_wait(barrier, total - 1)

    def to_left(slot):
        return pltpu.make_async_remote_copy(
            src_ref=out_l.at[slot], dst_ref=in_r.at[slot], send_sem=lsend.at[slot],
            recv_sem=lrecv.at[slot], device_id={"tm": (tm + n - 1) % n, "freq": fr},
            device_id_type=MESH)

    def to_right(slot):
        return pltpu.make_async_remote_copy(
            src_ref=out_r.at[slot], dst_ref=in_l.at[slot], send_sem=rsend.at[slot],
            recv_sem=rrecv.at[slot], device_id={"tm": (tm + 1) % n, "freq": fr},
            device_id_type=MESH)

    for slot in range(2):
        for devs, make in ((left[slot], to_left), (right[slot], to_right)):
            if devs:
                @pl.when(within(tm, devs))
                def _(make=make, slot=slot):
                    make(slot).start()

    for c in range(3):
        own[:, c * width : (c + 1) * width] = jnp.dot(
            t_ref[4 * ROWS :, :], xv[c], preferred_element_type=jnp.float32)

    def scatter(block, k):
        dest = (tm + k) % n
        return pltpu.make_async_remote_copy(
            src_ref=sendb.at[dest, block], dst_ref=recvb.at[tm, block],
            send_sem=asend.at[block, dest], recv_sem=arecv.at[block, tm],
            device_id={"tm": dest, "freq": fr}, device_id_type=MESH)

    order = list(range(2, per - 2)) + [1, per - 2, per - 1, 0]
    for block in order:
        span = slice(block * ROWS, (block + 1) * ROWS)
        if block < 2 and right[block]:
            @pl.when(within(tm - 1, right[block]))
            def _(block=block, span=span):
                to_right(block).wait_recv()
                own[span, :] += in_l[block]
        back = per - 1 - block
        if back < 2 and left[back]:
            @pl.when(within(tm + 1, left[back]))
            def _(back=back, span=span):
                to_left(back).wait_recv()
                own[span, :] += in_r[back]
        pw = width // n
        for dest in range(n):
            for c in range(3):
                sendb[dest, block, :, c * pw : (c + 1) * pw] = own[
                    span, c * width + dest * pw : c * width + (dest + 1) * pw].astype(jnp.bfloat16)

        @pl.loop(1, n)
        def _(k, block=block):
            scatter(block, k).start()

    def widen(src, block, values):
        base = (src * per + block) * ROWS
        for c in range(3):
            spec32[c, pl.ds(pl.multiple_of(base, ROWS), ROWS), :] = values[:, c * 128 : (c + 1) * 128].astype(jnp.float32)

    for block in range(per):
        widen(tm, block, sendb[tm, block])

    @pl.loop(1, n)
    def _(k):
        src = (tm + n - k) % n
        for block in range(per):
            pltpu.make_async_remote_copy(
                src_ref=sendb.at[src, block], dst_ref=recvb.at[src, block],
                send_sem=asend.at[block, src], recv_sem=arecv.at[block, src],
                device_id={"tm": src, "freq": fr}, device_id_type=MESH).wait_recv()
            widen(src, block, recvb[src, block])

    def to_owner(f):
        return pltpu.make_async_remote_copy(
            src_ref=gpart.at[f], dst_ref=gath.at[lin], send_sem=gsend.at[f],
            recv_sem=grecv.at[lin], device_id=where_is(f * stride), device_id_type=MESH)

    for f in range(NF):
        real = [spec32[c, pl.ds(2 * f, NB, stride=ROWS), :].astype(jnp.bfloat16) for c in range(3)]
        imag = [spec32[c, pl.ds(2 * f + 1, NB, stride=ROWS), :].astype(jnp.bfloat16) for c in range(3)]
        for c in range(3):
            spec[f, c * 2 * NB : c * 2 * NB + NB, :] = real[c]
            spec[f, c * 2 * NB + NB : (c + 1) * 2 * NB, :] = imag[c]
        lhs = jnp.concatenate(real + imag, axis=1)
        rhs = jnp.concatenate([lhs, jnp.concatenate(imag + [-v for v in real], axis=1)], axis=0)
        gram = lax.dot_general(lhs, rhs, (((1,), (1,)), ((), ())), preferred_element_type=jnp.float32)
        half = NB // 2
        gpart[f] = jnp.concatenate([gram[:half], gram[half:]], axis=1)
        if f % 4 == 3:
            for sent in range(f - 3, f + 1):
                @pl.when(lin != sent * stride)
                def _(sent=sent):
                    to_owner(sent).start()

    def coef_to(index):
        return pltpu.make_async_remote_copy(
            src_ref=msg, dst_ref=crecv.at[lin // stride], send_sem=csend.at[index],
            recv_sem=crcv.at[lin // stride], device_id=where_is(index), device_id_type=MESH)

    @pl.when(lin % stride == 0)
    def _():
        f_mine = lin // stride
        gath[lin] = gpart[f_mine]

        @pl.loop(1, total)
        def _(k):
            src = (lin + k) % total
            pltpu.make_async_remote_copy(
                src_ref=gpart.at[0], dst_ref=gath.at[src], send_sem=gsend.at[0],
                recv_sem=grecv.at[src], device_id=where_is(src), device_id_type=MESH).wait_recv()

        packed = jnp.sum(gath[...], axis=0)
        both = jnp.concatenate([packed[:, : 2 * NB], packed[:, 2 * NB :]], axis=0)
        gram_re = both[:, :NB]
        gram_im = both[:, NB:]
        hermit = jnp.concatenate([
            jnp.concatenate([gram_re, -gram_im], axis=1),
            jnp.concatenate([gram_im, gram_re], axis=1)], axis=0)
        frob = jnp.sqrt(jnp.sum(hermit * hermit, axis=(0, 1), keepdims=True) + 1e-06)
        ri = lax.broadcasted_iota(jnp.int32, (2 * NB, 2 * NB), 0)
        ci = lax.broadcasted_iota(jnp.int32, (2 * NB, 2 * NB), 1)
        identity = jnp.where(ri == ci, 1.0, 0.0).astype(jnp.float32)
        energy = jnp.sum(jnp.where((ri == ci) & (ri < NB), hermit, 0.0), axis=(0, 1), keepdims=True) / (3.0 * NB * points)

        def mul(a, b):
            return jnp.dot(a, b, precision=lax.Precision.HIGHEST, preferred_element_type=jnp.float32)

        iterate = hermit / frob
        inverse = identity
        for step in range(NSIT):
            factor = 1.5 * identity - 0.5 * (iterate if step == 0 else mul(inverse, iterate))
            if step < NSIT - 1:
                iterate = mul(iterate, factor)
                inverse = factor if step == 0 else mul(factor, inverse)
            else:
                inverse = mul(factor[:NB], inverse)
        scaled = inverse[:NB] * jnp.sqrt(6.0 * points / frob)
        upper = scaled[:, :NB]
        lower = scaled[:, NB:]
        msg[:NB, :] = jnp.concatenate([upper, -lower, lower, upper], axis=1).astype(jnp.bfloat16)
        high = energy.astype(jnp.bfloat16).astype(jnp.float32)
        lane = lax.broadcasted_iota(jnp.int32, (16, 128), 1)
        tail = jnp.where(lane == 0, high, jnp.where(lane == 1, energy - high, 0.0))
        msg[NB:, :] = tail.astype(jnp.bfloat16)
        crecv[f_mine] = msg[...]

        @pl.loop(1, total)
        def _(k):
            coef_to((lin + k) % total).start()

    for f in range(NF):
        @pl.when(lin != f * stride)
        def _(f=f):
            pltpu.make_async_remote_copy(
                src_ref=msg, dst_ref=crecv.at[f], send_sem=csend.at[f], recv_sem=crcv.at[f],
                device_id=where_is(f * stride), device_id_type=MESH).wait_recv()

    for f in range(NF):
        pairs = crecv[f, :NB, :]
        stacked = jnp.concatenate([pairs[:, : 2 * NB], pairs[:, 2 * NB :]], axis=0)
        tiled = jnp.concatenate([stacked] * 3, axis=1)
        full = jnp.dot(spread_ref[...], tiled, preferred_element_type=jnp.float32)
        full = (full * mask_ref[...]).astype(jnp.bfloat16)
        modes_ref[f * 6 * NB : (f + 1) * 6 * NB, :] = jnp.dot(
            full, spec[f], preferred_element_type=jnp.float32).astype(jnp.bfloat16)
        tail = crecv[f, NB:, :].astype(jnp.float32)
        energy_ref[f : f + 1, :] = jnp.broadcast_to(jnp.sum(tail[:1, :], axis=1, keepdims=True), (1, 128))

    for slot in range(2):
        for devs, make in ((left[slot], to_left), (right[slot], to_right)):
            if devs:
                @pl.when(within(tm, devs))
                def _(make=make, slot=slot):
                    make(slot).wait_send()

    @pl.loop(1, n)
    def _(k):
        for block in range(per):
            scatter(block, k).wait_send()

    for f in range(NF):
        @pl.when(lin != f * stride)
        def _(f=f):
            to_owner(f).wait_send()

    @pl.when(lin % stride == 0)
    def _():
        @pl.loop(1, total)
        def _(k):
            coef_to((lin + k) % total).wait_send()


def fused(n, nf_dev, chosen, snapshots, block_starts, freq_index):
    per, left, right = chosen
    rows, count, wide = snapshots.shape
    total = n * nf_dev
    pw = wide // n
    f32, bf16 = jnp.float32, jnp.bfloat16
    dma = pltpu.SemaphoreType.DMA
    vmem = pl.BlockSpec(memory_space=pltpu.VMEM)
    smem = pl.BlockSpec(memory_space=pltpu.SMEM)
    modes, energy = pl.pallas_call(
        functools.partial(kernel, n, nf_dev, per, left, right, float(wide * nf_dev)),
        out_shape=(jax.ShapeDtypeStruct((NF * NB * 6, pw), bf16), jax.ShapeDtypeStruct((NF, 128), f32)),
        in_specs=[pl.BlockSpec(memory_space=pltpu.HBM), smem, smem],
        out_specs=(vmem, vmem),
        scratch_shapes=[
            pltpu.VMEM(((per + 4) * ROWS, rows), bf16),
            pltpu.VMEM((NB * 6, 2 * NB), bf16),
            pltpu.VMEM((NB * 6, 6 * NB), f32),
            pltpu.VMEM((3, rows, wide), bf16),
            pltpu.VMEM((2, ROWS, 3 * wide), f32),
            pltpu.VMEM((2, ROWS, 3 * wide), f32),
            pltpu.VMEM((2, ROWS, 3 * wide), f32),
            pltpu.VMEM((2, ROWS, 3 * wide), f32),
            pltpu.VMEM((per * ROWS, 3 * wide), f32),
            pltpu.VMEM((n, per, ROWS, 3 * pw), bf16),
            pltpu.VMEM((n, per, ROWS, 3 * pw), bf16),
            pltpu.VMEM((3, NB * ROWS, pw), f32),
            pltpu.VMEM((NF, 6 * NB, pw), bf16),
            pltpu.VMEM((NF, NB // 2, 4 * NB), f32),
            pltpu.VMEM((total, NB // 2, 4 * NB), f32),
            pltpu.VMEM((NB + 16, 4 * NB), bf16),
            pltpu.VMEM((NF, NB + 16, 4 * NB), bf16),
            dma((3,)), dma((2,)), dma((2,)), dma((2,)), dma((2,)),
            dma((per, n)), dma((per, n)), dma((NF,)), dma((total,)), dma((total,)), dma((NF,)),
        ],
        compiler_params=pltpu.CompilerParams(
            collective_id=0, has_side_effects=True, vmem_limit_bytes=48 * 1024 * 1024),
    )(jnp.transpose(snapshots, (1, 0, 2)), block_starts, freq_index)
    modes = modes.reshape(NF, NB, 3, 2, pw).transpose(0, 1, 3, 2, 4)
    return modes, energy[:, 0]


def solution(mesh):
    n, nf_dev = mesh.shape["tm"], mesh.shape["freq"]

    def body(snapshots, block_starts, freq_index):
        rows, _, wide = snapshots.shape
        chosen = plan(n, rows, n * nf_dev, wide // n)
        if chosen is None:
            return local(snapshots, block_starts, freq_index)
        return fused(n, nf_dev, chosen, snapshots, block_starts, freq_index)

    return jax.shard_map(
        body,
        mesh=mesh,
        in_specs=(P("tm", None, "freq"), P(), P()),
        out_specs=(P(None, None, None, None, ("freq", "tm")), P()),
        check_vma=False,
    )
```

```python
import functools
import math

import jax
import jax.numpy as jnp
import numpy as np
from jax import lax
from jax.experimental import pallas as pl
from jax.experimental.pallas import tpu as pltpu
from jax.sharding import PartitionSpec as P

NB = 32
NFFT = 256
NF = 16
NSIT = 6


def for_sending(shard):
    return jax.tree.map(lambda a: a.astype(jnp.bfloat16) if a.dtype == jnp.float32 else a, shard)


def dft_rows(freq_index):
    times_idx = jnp.arange(NFFT, dtype=jnp.int32)
    phase_int = freq_index[:, None] * times_idx[None, :] % NFFT
    angles = 2.0 * math.pi / NFFT * phase_int.astype(jnp.float32)
    window = 0.5 - 0.5 * jnp.cos(2.0 * math.pi / NFFT * times_idx.astype(jnp.float32))
    scaling = 1.0 / jnp.sqrt(jnp.sum(window * window))
    cosine = window[None, :] * jnp.cos(angles) * scaling
    sine_rows = -window[None, :] * jnp.sin(angles) * scaling
    return jnp.stack([cosine, sine_rows], 1).reshape(2 * NF, NFFT).astype(jnp.bfloat16)


def block_rows(block_starts):
    return block_starts[:, None] + jnp.arange(NFFT, dtype=jnp.int32)[None, :]


def matmul_batch(left, right):
    return jnp.einsum("fij,fjk->fik", left, right, precision=lax.Precision.HIGHEST)


def whiten(summed, points):
    gram_re = summed[:, 0]
    gram_im = summed[:, 1]
    top_rows = jnp.concatenate([gram_re, -gram_im], 2)
    low_rows = jnp.concatenate([gram_im, gram_re], 2)
    hermit = jnp.concatenate([top_rows, low_rows], 1)
    frob = jnp.sqrt(jnp.sum(hermit * hermit, axis=(1, 2)) + 1e-06)
    identity = jnp.eye(2 * NB, dtype=jnp.float32)[None]
    iterate = hermit / frob[:, None, None]
    inverse = jnp.broadcast_to(identity, hermit.shape)
    for iteration in range(NSIT):
        factor = 1.5 * identity - 0.5 * matmul_batch(inverse, iterate)
        iterate = matmul_batch(iterate, factor)
        inverse = matmul_batch(factor, inverse)
    columns = inverse[:, :, :NB] * jnp.sqrt(6.0 * points / frob)[:, None, None]
    upper = columns[:, :NB]
    lower = columns[:, NB:]
    coefficients = jnp.stack([jnp.stack([upper, -lower], 1), jnp.stack([lower, upper], 1)], 1)
    energy = jnp.trace(gram_re, axis1=1, axis2=2) / (3.0 * NB * points)
    return (coefficients, energy)


def local(snapshots, block_starts, freq_index):
    dft_table = dft_rows(freq_index)
    offsets = block_rows(block_starts)
    series = lax.all_to_all(snapshots, "tm", split_axis=2, concat_axis=0, tiled=True)
    count = series.shape[1]
    width = series.shape[2]
    columns_all = series.reshape(series.shape[0], count * width)
    windows = jnp.take(columns_all, offsets, axis=0)
    spectra_part = jnp.einsum(
        "rt,btn->rbn", dft_table, windows, preferred_element_type=jnp.float32
    ).astype(jnp.bfloat16)
    spectra = spectra_part.reshape(2 * NF, NB, count, width)
    width = spectra.shape[3]
    points = float(width * lax.axis_size("tm") * lax.axis_size("freq"))
    flat_spec = spectra.reshape(NF, 2, NB, 3 * width)
    real_part = flat_spec[:, 0]
    imag_part = flat_spec[:, 1]
    gram_re = jnp.einsum("fbn,fcn->fbc", real_part, real_part, preferred_element_type=jnp.float32)
    gram_re = gram_re + jnp.einsum(
        "fbn,fcn->fbc", imag_part, imag_part, preferred_element_type=jnp.float32
    )
    cross_terms = jnp.einsum(
        "fbn,fcn->fbc", real_part, imag_part, preferred_element_type=jnp.float32
    )
    partial_gram = jnp.stack([gram_re, cross_terms - jnp.swapaxes(cross_terms, 1, 2)], 1)
    shared = lax.psum_scatter(partial_gram, "freq", scatter_dimension=0, tiled=True)
    shared = lax.psum(shared, "tm")
    coef_part, energy_part = whiten(shared, points)
    coefficients, energy = (
        lax.all_gather(for_sending(coef_part), "freq", axis=0, tiled=True).astype(coef_part.dtype),
        lax.all_gather(for_sending(energy_part), "freq", axis=0, tiled=True).astype(
            energy_part.dtype
        ),
    )
    coef_bf = jnp.transpose(coefficients.astype(jnp.bfloat16), (0, 4, 1, 2, 3))
    modes = jnp.einsum(
        "fjorb,frbn->fjon", coef_bf, flat_spec, preferred_element_type=jnp.float32
    ).astype(jnp.bfloat16)
    return (modes.reshape(NF, NB, 2, 3, width), energy)


MESH = pl.DeviceIdType.MESH
ROWS = 2 * NF
HOP = 128
JIT = 64


def plan(n, rows, total, width):
    if n < 2 or n % 2 or NB % n or total % NF or width != 128 or rows % 16:
        return None
    per = NB // n
    if per < 4 or per % 2:
        return None
    slots = per + 4
    whole = [[] for _ in range(slots)]
    shared = [[] for _ in range(slots)]
    holders = []
    for block in range(NB):
        touched = [
            dev for dev in range(n)
            if HOP * block < rows * (dev + 1) and HOP * block + JIT + NFFT > rows * dev
        ]
        holders.append(touched)
        if len(touched) > 2:
            return None
        for dev in touched:
            slot = block - per * dev + 2
            if not 0 <= slot < slots:
                return None
            if len(touched) == 2:
                if (slot < slots // 2) != (dev == touched[1]):
                    return None
                shared[slot].append(dev)
            else:
                whole[slot].append(dev)
    return per, whole, shared, holders


def base_table(freq_ref):
    row = lax.broadcasted_iota(jnp.int32, (ROWS, NFFT), 0)
    times_idx = lax.broadcasted_iota(jnp.int32, (ROWS, NFFT), 1)
    freqs = jnp.zeros((ROWS, NFFT), jnp.int32)
    for f in range(NF):
        freqs = jnp.where((row >> 1) == f, freq_ref[f], freqs)
    phase = (freqs * times_idx) & (NFFT - 1)
    angles = 2.0 * math.pi / NFFT * phase.astype(jnp.float32)
    window = 0.5 - 0.5 * jnp.cos(2.0 * math.pi / NFFT * times_idx.astype(jnp.float32))
    hann = 0.5 - 0.5 * np.cos(2.0 * math.pi / NFFT * np.arange(NFFT))
    scaling = np.float32(1.0 / np.sqrt(np.sum(hann * hann)))
    cosine = window * jnp.cos(angles) * scaling
    sine = -window * jnp.sin(angles) * scaling
    return jnp.where((row & 1) == 1, sine, cosine).astype(jnp.bfloat16)


def shifted(base, shift, rows):
    source = lax.broadcasted_iota(jnp.int32, (NFFT, rows), 0)
    target = lax.broadcasted_iota(jnp.int32, (NFFT, rows), 1)
    pick = jnp.where(source - target == shift, 1.0, 0.0).astype(jnp.bfloat16)
    return jnp.dot(base, pick, preferred_element_type=jnp.float32).astype(jnp.bfloat16)


def expanders(spread_ref, mask_ref):
    row = lax.broadcasted_iota(jnp.int32, (NB * 6, 2 * NB), 0)
    col = lax.broadcasted_iota(jnp.int32, (NB * 6, 2 * NB), 1)
    first = 6 * (col & (NB - 1))
    hit = (row >= first) & (row < first + 6) & ((row & 1) == jnp.where(col >= NB, 1, 0))
    spread_ref[...] = jnp.where(hit, 1.0, 0.0).astype(jnp.bfloat16)
    row = lax.broadcasted_iota(jnp.int32, (NB * 6, 6 * NB), 0)
    col = lax.broadcasted_iota(jnp.int32, (NB * 6, 6 * NB), 1)
    pair = row >> 1
    comp = pair - 3 * ((pair * 43691) >> 17)
    part = jnp.where(col >= 4 * NB, 2, jnp.where(col >= 2 * NB, 1, 0))
    mask_ref[...] = jnp.where(comp == part, 1.0, 0.0)


def member(index, devs):
    if not devs:
        return None
    if devs == list(range(devs[0], devs[-1] + 1)):
        return (index >= devs[0]) & (index <= devs[-1])
    hit = index == devs[0]
    for dev in devs[1:]:
        hit = hit | (index == dev)
    return hit


def kernel(n, nf_dev, per, whole, shared, holders, points, x_hbm, starts_hbm, freq_hbm,
           modes_ref, energy_ref, starts_ref, freq_ref, t_ref, spread_ref, mask_ref, xv, parts,
           others, sendb, recvb, spec32, spec, gpart, gath, msg, crecv, load_sem, psend, precv,
           asend, arecv, gsend, grecv, csend, crcv):
    tm = lax.axis_index("tm")
    fr = lax.axis_index("freq")
    total = n * nf_dev
    lin = tm * nf_dev + fr
    stride = total // NF
    slots = per + 4
    half_n = n // 2
    parity = tm % 2

    def where_is(index):
        return {"tm": index // nf_dev, "freq": index % nf_dev}

    small = [
        pltpu.make_async_copy(starts_hbm, starts_ref, load_sem.at[3]),
        pltpu.make_async_copy(freq_hbm, freq_ref, load_sem.at[4]),
    ]
    for copy in small:
        copy.start()
    for c in range(3):
        pltpu.make_async_copy(x_hbm.at[c], xv.at[c], load_sem.at[c]).start()
    barrier = pltpu.get_barrier_semaphore()

    @pl.loop(1, total)
    def _(k):
        pl.semaphore_signal(barrier, inc=1, device_id=where_is((lin + k) % total), device_id_type=MESH)

    for copy in small:
        copy.wait()
    rows = xv.shape[1]
    base = base_table(freq_ref)
    for slot in range(slots):
        block = per * tm + slot - 2
        start = starts_ref[jnp.clip(block, 0, NB - 1)]
        inside = (block >= 0) & (block < NB)
        shift = jnp.where(inside, rows * tm - start, 4 * (rows + NFFT))
        t_ref[slot * ROWS : (slot + 1) * ROWS, :] = shifted(base, shift, rows)
    expanders(spread_ref, mask_ref)
    width = xv.shape[2]
    pw = width // n
    for c in range(3):
        pltpu.make_async_copy(x_hbm.at[c], xv.at[c], load_sem.at[c]).wait()
        part = jnp.dot(t_ref[...], xv[c], preferred_element_type=jnp.float32)
        for slot in range(slots):
            for dest in range(n):
                at = (c * half_n + dest // 2) * pw
                parts[slot, dest % 2, :, at : at + pw] = part[
                    slot * ROWS : (slot + 1) * ROWS, dest * pw : (dest + 1) * pw]
    pl.semaphore_wait(barrier, total - 1)

    def exchange(slot):
        low = slot < slots // 2
        return pltpu.make_async_remote_copy(
            src_ref=parts.at[slot, 1 - parity], dst_ref=others.at[slot + per if low else slot - per],
            send_sem=psend.at[slot], recv_sem=precv.at[slot + per if low else slot - per],
            device_id={"tm": (tm + n - 1) % n if low else (tm + 1) % n, "freq": fr},
            device_id_type=MESH)

    def arrival(slot):
        return pltpu.make_async_remote_copy(
            src_ref=parts.at[slot, 1 - parity], dst_ref=others.at[slot],
            send_sem=psend.at[slot], recv_sem=precv.at[slot],
            device_id={"tm": tm, "freq": fr}, device_id_type=MESH)

    outward = []
    for step in range(slots // 2):
        outward += [(slots // 2 + step) % slots, slots // 2 - 1 - step]
    inward = [slot + per if slot < slots // 2 else slot - per for slot in outward]

    for slot in outward:
        if shared[slot]:
            @pl.when(member(tm, shared[slot]))
            def _(slot=slot):
                exchange(slot).start()

    def scatter(slot, dest):
        return pltpu.make_async_remote_copy(
            src_ref=sendb.at[slot, dest], dst_ref=recvb.at[per * tm + slot - 2],
            send_sem=asend.at[slot, dest], recv_sem=arecv.at[per * tm + slot - 2],
            device_id={"tm": dest, "freq": fr}, device_id_type=MESH)

    def same_side(k):
        return 2 * ((tm // 2 + k) % half_n) + parity

    def other_side(k):
        return 2 * ((tm // 2 + k) % half_n) + 1 - parity

    def finish(slot, side, add):
        for q in range(half_n):
            for c in range(3):
                at = (c * half_n + q) * pw
                value = parts[slot, side, :, at : at + pw]
                if add:
                    value = value + others[slot, :, at : at + pw]
                sendb[slot, 2 * q + side, :, c * pw : (c + 1) * pw] = value.astype(jnp.bfloat16)

    def keep(slot):
        recvb[per * tm + slot - 2] = sendb[slot, tm]

    for slot in range(slots):
        if whole[slot]:
            @pl.when(member(tm, whole[slot]))
            def _(slot=slot):
                finish(slot, parity, False)
                finish(slot, 1 - parity, False)

                @pl.loop(1, half_n)
                def _(k):
                    scatter(slot, same_side(k)).start()

                @pl.loop(0, half_n)
                def _(k):
                    scatter(slot, other_side(k)).start()

                keep(slot)

    for slot in inward:
        if shared[slot]:
            @pl.when(member(tm, shared[slot]))
            def _(slot=slot):
                arrival(slot).wait_recv()
                finish(slot, parity, True)

                @pl.loop(1, half_n)
                def _(k):
                    scatter(slot, same_side(k)).start()

                keep(slot)

    ordered = [b for b in range(NB) if len(holders[b]) == 1] + [b for b in range(NB) if len(holders[b]) == 2]
    for block in ordered:
        @pl.when(jnp.logical_not(member(tm, holders[block])))
        def _(block=block):
            pltpu.make_async_remote_copy(
                src_ref=sendb.at[0, 0], dst_ref=recvb.at[block], send_sem=asend.at[0, 0],
                recv_sem=arecv.at[block], device_id={"tm": tm, "freq": fr},
                device_id_type=MESH).wait_recv()

    for block in range(NB):
        values = recvb[block]
        for c in range(3):
            spec32[c, block * ROWS : (block + 1) * ROWS, :] = values[:, c * 128 : (c + 1) * 128].astype(jnp.float32)

    def to_owner(f):
        return pltpu.make_async_remote_copy(
            src_ref=gpart.at[f], dst_ref=gath.at[lin], send_sem=gsend.at[f],
            recv_sem=grecv.at[lin], device_id=where_is(f * stride), device_id_type=MESH)

    for f in range(NF):
        real = [spec32[c, pl.ds(2 * f, NB, stride=ROWS), :].astype(jnp.bfloat16) for c in range(3)]
        imag = [spec32[c, pl.ds(2 * f + 1, NB, stride=ROWS), :].astype(jnp.bfloat16) for c in range(3)]
        for c in range(3):
            spec[f, c * 2 * NB : c * 2 * NB + NB, :] = real[c]
            spec[f, c * 2 * NB + NB : (c + 1) * 2 * NB, :] = imag[c]
        lhs = jnp.concatenate(real + imag, axis=1)
        rhs = jnp.concatenate([lhs, jnp.concatenate(imag + [-v for v in real], axis=1)], axis=0)
        gram = lax.dot_general(lhs, rhs, (((1,), (1,)), ((), ())), preferred_element_type=jnp.float32)
        half = NB // 2
        gpart[f] = jnp.concatenate([gram[:half], gram[half:]], axis=1)
        if f % 4 == 3:
            for sent in range(f - 3, f + 1):
                @pl.when(lin != sent * stride)
                def _(sent=sent):
                    to_owner(sent).start()

    def coef_to(index):
        return pltpu.make_async_remote_copy(
            src_ref=msg, dst_ref=crecv.at[lin // stride], send_sem=csend.at[index],
            recv_sem=crcv.at[lin // stride], device_id=where_is(index), device_id_type=MESH)

    @pl.when(lin % stride == 0)
    def _():
        f_mine = lin // stride
        gath[lin] = gpart[f_mine]

        @pl.loop(1, total)
        def _(k):
            src = (lin + k) % total
            pltpu.make_async_remote_copy(
                src_ref=gpart.at[0], dst_ref=gath.at[src], send_sem=gsend.at[0],
                recv_sem=grecv.at[src], device_id=where_is(src), device_id_type=MESH).wait_recv()

        packed = jnp.sum(gath[...], axis=0)
        both = jnp.concatenate([packed[:, : 2 * NB], packed[:, 2 * NB :]], axis=0)
        gram_re = both[:, :NB]
        gram_im = both[:, NB:]
        hermit = jnp.concatenate([
            jnp.concatenate([gram_re, -gram_im], axis=1),
            jnp.concatenate([gram_im, gram_re], axis=1)], axis=0)
        frob = jnp.sqrt(jnp.sum(hermit * hermit, axis=(0, 1), keepdims=True) + 1e-06)
        ri = lax.broadcasted_iota(jnp.int32, (2 * NB, 2 * NB), 0)
        ci = lax.broadcasted_iota(jnp.int32, (2 * NB, 2 * NB), 1)
        identity = jnp.where(ri == ci, 1.0, 0.0).astype(jnp.float32)
        energy = jnp.sum(jnp.where((ri == ci) & (ri < NB), hermit, 0.0), axis=(0, 1), keepdims=True) / (3.0 * NB * points)

        def mul(a, b):
            return jnp.dot(a, b, precision=lax.Precision.HIGHEST, preferred_element_type=jnp.float32)

        iterate = hermit / frob
        inverse = identity
        for step in range(NSIT):
            factor = 1.5 * identity - 0.5 * (iterate if step == 0 else mul(inverse, iterate))
            if step < NSIT - 1:
                iterate = mul(iterate, factor)
                inverse = factor if step == 0 else mul(factor, inverse)
            else:
                inverse = mul(factor[:NB], inverse)
        scaled = inverse[:NB] * jnp.sqrt(6.0 * points / frob)
        upper = scaled[:, :NB]
        lower = scaled[:, NB:]
        msg[:NB, :] = jnp.concatenate([upper, -lower, lower, upper], axis=1).astype(jnp.bfloat16)
        high = energy.astype(jnp.bfloat16).astype(jnp.float32)
        lane = lax.broadcasted_iota(jnp.int32, (16, 128), 1)
        tail = jnp.where(lane == 0, high, jnp.where(lane == 1, energy - high, 0.0))
        msg[NB:, :] = tail.astype(jnp.bfloat16)
        crecv[f_mine] = msg[...]

        @pl.loop(1, total)
        def _(k):
            coef_to((lin + k) % total).start()

    for f in range(NF):
        @pl.when(lin != f * stride)
        def _(f=f):
            pltpu.make_async_remote_copy(
                src_ref=msg, dst_ref=crecv.at[f], send_sem=csend.at[f], recv_sem=crcv.at[f],
                device_id=where_is(f * stride), device_id_type=MESH).wait_recv()

    for f in range(NF):
        pairs = crecv[f, :NB, :]
        stacked = jnp.concatenate([pairs[:, : 2 * NB], pairs[:, 2 * NB :]], axis=0)
        tiled = jnp.concatenate([stacked] * 3, axis=1)
        full = jnp.dot(spread_ref[...], tiled, preferred_element_type=jnp.float32)
        full = (full * mask_ref[...]).astype(jnp.bfloat16)
        modes_ref[f * 6 * NB : (f + 1) * 6 * NB, :] = jnp.dot(
            full, spec[f], preferred_element_type=jnp.float32).astype(jnp.bfloat16)
        tail = crecv[f, NB:, :].astype(jnp.float32)
        energy_ref[f : f + 1, :] = jnp.broadcast_to(jnp.sum(tail[:1, :], axis=1, keepdims=True), (1, 128))

    for slot in range(slots):
        if shared[slot]:
            @pl.when(member(tm, shared[slot]))
            def _(slot=slot):
                exchange(slot).wait_send()

                @pl.loop(1, half_n)
                def _(k):
                    scatter(slot, same_side(k)).wait_send()

        if whole[slot]:
            @pl.when(member(tm, whole[slot]))
            def _(slot=slot):
                @pl.loop(1, half_n)
                def _(k):
                    scatter(slot, same_side(k)).wait_send()

                @pl.loop(0, half_n)
                def _(k):
                    scatter(slot, other_side(k)).wait_send()

    for f in range(NF):
        @pl.when(lin != f * stride)
        def _(f=f):
            to_owner(f).wait_send()

    @pl.when(lin % stride == 0)
    def _():
        @pl.loop(1, total)
        def _(k):
            coef_to((lin + k) % total).wait_send()


def fused(n, nf_dev, chosen, snapshots, block_starts, freq_index):
    per, whole, shared, holders = chosen
    rows, count, wide = snapshots.shape
    total = n * nf_dev
    pw = wide // n
    slots = per + 4
    f32, bf16 = jnp.float32, jnp.bfloat16
    dma = pltpu.SemaphoreType.DMA
    vmem = pl.BlockSpec(memory_space=pltpu.VMEM)
    modes, energy = pl.pallas_call(
        functools.partial(kernel, n, nf_dev, per, whole, shared, holders, float(wide * nf_dev)),
        out_shape=(jax.ShapeDtypeStruct((NF * NB * 6, pw), bf16), jax.ShapeDtypeStruct((NF, 128), f32)),
        in_specs=[pl.BlockSpec(memory_space=pltpu.HBM)] * 3,
        out_specs=(vmem, vmem),
        scratch_shapes=[
            pltpu.SMEM((NB,), jnp.int32),
            pltpu.SMEM((NF,), jnp.int32),
            pltpu.VMEM((slots * ROWS, rows), bf16),
            pltpu.VMEM((NB * 6, 2 * NB), bf16),
            pltpu.VMEM((NB * 6, 6 * NB), f32),
            pltpu.VMEM((3, rows, wide), bf16),
            pltpu.VMEM((slots, 2, ROWS, 3 * wide // 2), f32),
            pltpu.VMEM((slots, ROWS, 3 * wide // 2), f32),
            pltpu.VMEM((slots, n, ROWS, 3 * pw), bf16),
            pltpu.VMEM((NB, ROWS, 3 * pw), bf16),
            pltpu.VMEM((3, NB * ROWS, pw), f32),
            pltpu.VMEM((NF, 6 * NB, pw), bf16),
            pltpu.VMEM((NF, NB // 2, 4 * NB), f32),
            pltpu.VMEM((total, NB // 2, 4 * NB), f32),
            pltpu.VMEM((NB + 16, 4 * NB), bf16),
            pltpu.VMEM((NF, NB + 16, 4 * NB), bf16),
            dma((5,)), dma((slots,)), dma((slots,)), dma((slots, n)), dma((NB,)),
            dma((NF,)), dma((total,)), dma((total,)), dma((NF,)),
        ],
        compiler_params=pltpu.CompilerParams(
            collective_id=0, has_side_effects=True, vmem_limit_bytes=60 * 1024 * 1024),
    )(jnp.transpose(snapshots, (1, 0, 2)), block_starts, freq_index)
    modes = modes.reshape(NF, NB, 3, 2, pw).transpose(0, 1, 3, 2, 4)
    return modes, energy[:, 0]


def solution(mesh):
    n, nf_dev = mesh.shape["tm"], mesh.shape["freq"]

    def body(snapshots, block_starts, freq_index):
        rows, _, wide = snapshots.shape
        chosen = plan(n, rows, n * nf_dev, wide // n)
        if chosen is None:
            return local(snapshots, block_starts, freq_index)
        return fused(n, nf_dev, chosen, snapshots, block_starts, freq_index)

    return jax.shard_map(
        body,
        mesh=mesh,
        in_specs=(P("tm", None, "freq"), P(), P()),
        out_specs=(P(None, None, None, None, ("freq", "tm")), P()),
        check_vma=False,
    )
```

```python
import functools
import math

import jax
import jax.numpy as jnp
import numpy as np
from jax import lax
from jax.experimental import pallas as pl
from jax.experimental.pallas import tpu as pltpu
from jax.sharding import PartitionSpec as P

NB = 32
NFFT = 256
NF = 16
NSIT = 6


def for_sending(shard):
    return jax.tree.map(lambda a: a.astype(jnp.bfloat16) if a.dtype == jnp.float32 else a, shard)


def dft_rows(freq_index):
    times_idx = jnp.arange(NFFT, dtype=jnp.int32)
    phase_int = freq_index[:, None] * times_idx[None, :] % NFFT
    angles = 2.0 * math.pi / NFFT * phase_int.astype(jnp.float32)
    window = 0.5 - 0.5 * jnp.cos(2.0 * math.pi / NFFT * times_idx.astype(jnp.float32))
    scaling = 1.0 / jnp.sqrt(jnp.sum(window * window))
    cosine = window[None, :] * jnp.cos(angles) * scaling
    sine_rows = -window[None, :] * jnp.sin(angles) * scaling
    return jnp.stack([cosine, sine_rows], 1).reshape(2 * NF, NFFT).astype(jnp.bfloat16)


def block_rows(block_starts):
    return block_starts[:, None] + jnp.arange(NFFT, dtype=jnp.int32)[None, :]


def matmul_batch(left, right):
    return jnp.einsum("fij,fjk->fik", left, right, precision=lax.Precision.HIGHEST)


def whiten(summed, points):
    gram_re = summed[:, 0]
    gram_im = summed[:, 1]
    top_rows = jnp.concatenate([gram_re, -gram_im], 2)
    low_rows = jnp.concatenate([gram_im, gram_re], 2)
    hermit = jnp.concatenate([top_rows, low_rows], 1)
    frob = jnp.sqrt(jnp.sum(hermit * hermit, axis=(1, 2)) + 1e-06)
    identity = jnp.eye(2 * NB, dtype=jnp.float32)[None]
    iterate = hermit / frob[:, None, None]
    inverse = jnp.broadcast_to(identity, hermit.shape)
    for iteration in range(NSIT):
        factor = 1.5 * identity - 0.5 * matmul_batch(inverse, iterate)
        iterate = matmul_batch(iterate, factor)
        inverse = matmul_batch(factor, inverse)
    columns = inverse[:, :, :NB] * jnp.sqrt(6.0 * points / frob)[:, None, None]
    upper = columns[:, :NB]
    lower = columns[:, NB:]
    coefficients = jnp.stack([jnp.stack([upper, -lower], 1), jnp.stack([lower, upper], 1)], 1)
    energy = jnp.trace(gram_re, axis1=1, axis2=2) / (3.0 * NB * points)
    return (coefficients, energy)


def local(snapshots, block_starts, freq_index):
    dft_table = dft_rows(freq_index)
    offsets = block_rows(block_starts)
    series = lax.all_to_all(snapshots, "tm", split_axis=2, concat_axis=0, tiled=True)
    count = series.shape[1]
    width = series.shape[2]
    columns_all = series.reshape(series.shape[0], count * width)
    windows = jnp.take(columns_all, offsets, axis=0)
    spectra_part = jnp.einsum(
        "rt,btn->rbn", dft_table, windows, preferred_element_type=jnp.float32
    ).astype(jnp.bfloat16)
    spectra = spectra_part.reshape(2 * NF, NB, count, width)
    width = spectra.shape[3]
    points = float(width * lax.axis_size("tm") * lax.axis_size("freq"))
    flat_spec = spectra.reshape(NF, 2, NB, 3 * width)
    real_part = flat_spec[:, 0]
    imag_part = flat_spec[:, 1]
    gram_re = jnp.einsum("fbn,fcn->fbc", real_part, real_part, preferred_element_type=jnp.float32)
    gram_re = gram_re + jnp.einsum(
        "fbn,fcn->fbc", imag_part, imag_part, preferred_element_type=jnp.float32
    )
    cross_terms = jnp.einsum(
        "fbn,fcn->fbc", real_part, imag_part, preferred_element_type=jnp.float32
    )
    partial_gram = jnp.stack([gram_re, cross_terms - jnp.swapaxes(cross_terms, 1, 2)], 1)
    shared = lax.psum_scatter(partial_gram, "freq", scatter_dimension=0, tiled=True)
    shared = lax.psum(shared, "tm")
    coef_part, energy_part = whiten(shared, points)
    coefficients, energy = (
        lax.all_gather(for_sending(coef_part), "freq", axis=0, tiled=True).astype(coef_part.dtype),
        lax.all_gather(for_sending(energy_part), "freq", axis=0, tiled=True).astype(
            energy_part.dtype
        ),
    )
    coef_bf = jnp.transpose(coefficients.astype(jnp.bfloat16), (0, 4, 1, 2, 3))
    modes = jnp.einsum(
        "fjorb,frbn->fjon", coef_bf, flat_spec, preferred_element_type=jnp.float32
    ).astype(jnp.bfloat16)
    return (modes.reshape(NF, NB, 2, 3, width), energy)


MESH = pl.DeviceIdType.MESH
ROWS = 2 * NF
HOP = 128
JIT = 64


def plan(n, rows, total, width):
    if n < 2 or n % 2 or NB % n or total % (2 * NF) or width != 128 or rows % 16:
        return None
    per = NB // n
    if per < 4 or per % 2:
        return None
    slots = per + 4
    whole = [[] for _ in range(slots)]
    shared = [[] for _ in range(slots)]
    holders = []
    for block in range(NB):
        touched = [
            dev for dev in range(n)
            if HOP * block < rows * (dev + 1) and HOP * block + JIT + NFFT > rows * dev
        ]
        holders.append(touched)
        if len(touched) > 2:
            return None
        for dev in touched:
            slot = block - per * dev + 2
            if not 0 <= slot < slots:
                return None
            if len(touched) == 2:
                if (slot < slots // 2) != (dev == touched[1]):
                    return None
                shared[slot].append(dev)
            else:
                whole[slot].append(dev)
    return per, whole, shared, holders


def base_table(freq_ref):
    row = lax.broadcasted_iota(jnp.int32, (ROWS, NFFT), 0)
    times_idx = lax.broadcasted_iota(jnp.int32, (ROWS, NFFT), 1)
    freqs = jnp.zeros((ROWS, NFFT), jnp.int32)
    for f in range(NF):
        freqs = jnp.where((row >> 1) == f, freq_ref[f], freqs)
    phase = (freqs * times_idx) & (NFFT - 1)
    angles = 2.0 * math.pi / NFFT * phase.astype(jnp.float32)
    window = 0.5 - 0.5 * jnp.cos(2.0 * math.pi / NFFT * times_idx.astype(jnp.float32))
    hann = 0.5 - 0.5 * np.cos(2.0 * math.pi / NFFT * np.arange(NFFT))
    scaling = np.float32(1.0 / np.sqrt(np.sum(hann * hann)))
    cosine = window * jnp.cos(angles) * scaling
    sine = -window * jnp.sin(angles) * scaling
    return jnp.where((row & 1) == 1, sine, cosine).astype(jnp.bfloat16)


def shifted(base, shift, rows):
    source = lax.broadcasted_iota(jnp.int32, (NFFT, rows), 0)
    target = lax.broadcasted_iota(jnp.int32, (NFFT, rows), 1)
    pick = jnp.where(source - target == shift, 1.0, 0.0).astype(jnp.bfloat16)
    return jnp.dot(base, pick, preferred_element_type=jnp.float32).astype(jnp.bfloat16)


def expanders(spread_ref, mask_ref):
    row = lax.broadcasted_iota(jnp.int32, (NB * 6, 2 * NB), 0)
    col = lax.broadcasted_iota(jnp.int32, (NB * 6, 2 * NB), 1)
    first = 6 * (col & (NB - 1))
    hit = (row >= first) & (row < first + 6) & ((row & 1) == jnp.where(col >= NB, 1, 0))
    spread_ref[...] = jnp.where(hit, 1.0, 0.0).astype(jnp.bfloat16)
    row = lax.broadcasted_iota(jnp.int32, (NB * 6, 6 * NB), 0)
    col = lax.broadcasted_iota(jnp.int32, (NB * 6, 6 * NB), 1)
    pair = row >> 1
    comp = pair - 3 * ((pair * 43691) >> 17)
    part = jnp.where(col >= 4 * NB, 2, jnp.where(col >= 2 * NB, 1, 0))
    mask_ref[...] = jnp.where(comp == part, 1.0, 0.0)


def member(index, devs):
    if not devs:
        return None
    if devs == list(range(devs[0], devs[-1] + 1)):
        return (index >= devs[0]) & (index <= devs[-1])
    hit = index == devs[0]
    for dev in devs[1:]:
        hit = hit | (index == dev)
    return hit


def kernel(n, nf_dev, per, whole, shared, holders, points, x_hbm, starts_hbm, freq_hbm,
           modes_ref, energy_ref, starts_ref, freq_ref, t_ref, spread_ref, mask_ref, xv, parts,
           others, sendb, recvb, spec32, spec, gpart, gath, msg, crecv, load_sem, psend, precv,
           asend, arecv, gsend, grecv, csend, crcv):
    tm = lax.axis_index("tm")
    fr = lax.axis_index("freq")
    total = n * nf_dev
    lin = tm * nf_dev + fr
    step, lowest = total // (2 * NF), total // 4
    slots = per + 4
    mine = (lin - lowest) // step
    owns = (lin >= lowest) & (lin < lowest + NF * step) & ((lin - lowest) % step == 0)
    half_n = n // 2
    parity = tm % 2

    def owner(f):
        return lowest + f * step

    def where_is(index):
        return {"tm": index // nf_dev, "freq": index % nf_dev}

    small = [
        pltpu.make_async_copy(starts_hbm, starts_ref, load_sem.at[3]),
        pltpu.make_async_copy(freq_hbm, freq_ref, load_sem.at[4]),
    ]
    for copy in small:
        copy.start()
    for c in range(3):
        pltpu.make_async_copy(x_hbm.at[c], xv.at[c], load_sem.at[c]).start()
    barrier = pltpu.get_barrier_semaphore()

    @pl.loop(1, total)
    def _(k):
        pl.semaphore_signal(barrier, inc=1, device_id=where_is((lin + k) % total), device_id_type=MESH)

    for copy in small:
        copy.wait()
    rows = xv.shape[1]
    base = base_table(freq_ref)
    for slot in range(slots):
        block = per * tm + slot - 2
        start = starts_ref[jnp.clip(block, 0, NB - 1)]
        inside = (block >= 0) & (block < NB)
        shift = jnp.where(inside, rows * tm - start, 4 * (rows + NFFT))
        t_ref[slot * ROWS : (slot + 1) * ROWS, :] = shifted(base, shift, rows)
    expanders(spread_ref, mask_ref)
    width = xv.shape[2]
    pw = width // n
    def exchange(slot, c):
        low = slot < slots // 2
        there = slot + per if low else slot - per
        return pltpu.make_async_remote_copy(
            src_ref=parts.at[slot, 1 - parity, c], dst_ref=others.at[there, c],
            send_sem=psend.at[slot, c], recv_sem=precv.at[there, c],
            device_id={"tm": (tm + n - 1) % n if low else (tm + 1) % n, "freq": fr},
            device_id_type=MESH)

    def arrival(slot, c):
        return pltpu.make_async_remote_copy(
            src_ref=parts.at[slot, 1 - parity, c], dst_ref=others.at[slot, c],
            send_sem=psend.at[slot, c], recv_sem=precv.at[slot, c],
            device_id={"tm": tm, "freq": fr}, device_id_type=MESH)

    outward = []
    for reach in range(slots // 2):
        outward += [slots // 2 + reach, slots // 2 - 1 - reach]
    inward = [slot + per if slot < slots // 2 else slot - per for slot in outward]

    pl.semaphore_wait(barrier, total - 1)

    for c in range(3):
        pltpu.make_async_copy(x_hbm.at[c], xv.at[c], load_sem.at[c]).wait()
        part = jnp.dot(t_ref[...], xv[c], preferred_element_type=jnp.float32)
        for slot in range(slots):
            for dest in range(n):
                at = dest // 2 * pw
                parts[slot, dest % 2, c, :, at : at + pw] = part[
                    slot * ROWS : (slot + 1) * ROWS, dest * pw : (dest + 1) * pw]
        for slot in outward:
            if shared[slot]:
                @pl.when(member(tm, shared[slot]))
                def _(slot=slot, c=c):
                    exchange(slot, c).start()

    def scatter(slot, dest):
        return pltpu.make_async_remote_copy(
            src_ref=sendb.at[slot, dest], dst_ref=recvb.at[per * tm + slot - 2],
            send_sem=asend.at[slot, dest], recv_sem=arecv.at[per * tm + slot - 2],
            device_id={"tm": dest, "freq": fr}, device_id_type=MESH)

    def same_side(k):
        return 2 * ((tm // 2 + k) % half_n) + parity

    def other_side(k):
        return 2 * ((tm // 2 + k) % half_n) + 1 - parity

    def finish(slot, side, add):
        for q in range(half_n):
            for c in range(3):
                at = q * pw
                value = parts[slot, side, c, :, at : at + pw]
                if add:
                    value = value + others[slot, c, :, at : at + pw]
                sendb[slot, 2 * q + side, :, c * pw : (c + 1) * pw] = value.astype(jnp.bfloat16)

    def keep(slot):
        recvb[per * tm + slot - 2] = sendb[slot, tm]

    for slot in range(slots):
        if whole[slot]:
            @pl.when(member(tm, whole[slot]))
            def _(slot=slot):
                finish(slot, parity, False)
                finish(slot, 1 - parity, False)

                @pl.loop(1, half_n)
                def _(k):
                    scatter(slot, same_side(k)).start()

                @pl.loop(0, half_n)
                def _(k):
                    scatter(slot, other_side(k)).start()

                keep(slot)

    for slot in inward:
        if shared[slot]:
            @pl.when(member(tm, shared[slot]))
            def _(slot=slot):
                for c in range(3):
                    arrival(slot, c).wait_recv()
                finish(slot, parity, True)

                @pl.loop(1, half_n)
                def _(k):
                    scatter(slot, same_side(k)).start()

                keep(slot)

    ordered = [b for b in range(NB) if len(holders[b]) == 1] + [b for b in range(NB) if len(holders[b]) == 2]
    for block in ordered:
        @pl.when(jnp.logical_not(member(tm, holders[block])))
        def _(block=block):
            pltpu.make_async_remote_copy(
                src_ref=sendb.at[0, 0], dst_ref=recvb.at[block], send_sem=asend.at[0, 0],
                recv_sem=arecv.at[block], device_id={"tm": tm, "freq": fr},
                device_id_type=MESH).wait_recv()

    for block in range(NB):
        values = recvb[block]
        for c in range(3):
            spec32[c, block * ROWS : (block + 1) * ROWS, :] = values[:, c * 128 : (c + 1) * 128].astype(jnp.float32)

    def to_owner(f):
        return pltpu.make_async_remote_copy(
            src_ref=gpart.at[f], dst_ref=gath.at[lin], send_sem=gsend.at[f],
            recv_sem=grecv.at[lin], device_id=where_is(owner(f)), device_id_type=MESH)

    for f in range(NF):
        real = [spec32[c, pl.ds(2 * f, NB, stride=ROWS), :].astype(jnp.bfloat16) for c in range(3)]
        imag = [spec32[c, pl.ds(2 * f + 1, NB, stride=ROWS), :].astype(jnp.bfloat16) for c in range(3)]
        for c in range(3):
            spec[f, c * 2 * NB : c * 2 * NB + NB, :] = real[c]
            spec[f, c * 2 * NB + NB : (c + 1) * 2 * NB, :] = imag[c]
        lhs = jnp.concatenate(real + imag, axis=1)
        rhs = jnp.concatenate([lhs, jnp.concatenate(imag + [-v for v in real], axis=1)], axis=0)
        gram = lax.dot_general(lhs, rhs, (((1,), (1,)), ((), ())), preferred_element_type=jnp.float32)
        half = NB // 2
        gpart[f] = jnp.concatenate([gram[:half], gram[half:]], axis=1)
        if f % 4 == 3:
            for sent in range(f - 3, f + 1):
                @pl.when(lin != owner(sent))
                def _(sent=sent):
                    to_owner(sent).start()

    def coef_to(index):
        return pltpu.make_async_remote_copy(
            src_ref=msg, dst_ref=crecv.at[mine], send_sem=csend.at[index],
            recv_sem=crcv.at[mine], device_id=where_is(index), device_id_type=MESH)

    @pl.when(owns)
    def _():
        gath[lin] = gpart[mine]

        @pl.loop(1, total)
        def _(k):
            src = (lin + k) % total
            pltpu.make_async_remote_copy(
                src_ref=gpart.at[0], dst_ref=gath.at[src], send_sem=gsend.at[0],
                recv_sem=grecv.at[src], device_id=where_is(src), device_id_type=MESH).wait_recv()

        packed = jnp.sum(gath[...], axis=0)
        both = jnp.concatenate([packed[:, : 2 * NB], packed[:, 2 * NB :]], axis=0)
        gram_re = both[:, :NB]
        gram_im = both[:, NB:]
        hermit = jnp.concatenate([
            jnp.concatenate([gram_re, -gram_im], axis=1),
            jnp.concatenate([gram_im, gram_re], axis=1)], axis=0)
        frob = jnp.sqrt(jnp.sum(hermit * hermit, axis=(0, 1), keepdims=True) + 1e-06)
        ri = lax.broadcasted_iota(jnp.int32, (2 * NB, 2 * NB), 0)
        ci = lax.broadcasted_iota(jnp.int32, (2 * NB, 2 * NB), 1)
        identity = jnp.where(ri == ci, 1.0, 0.0).astype(jnp.float32)
        energy = jnp.sum(jnp.where((ri == ci) & (ri < NB), hermit, 0.0), axis=(0, 1), keepdims=True) / (3.0 * NB * points)

        def mul(a, b):
            return jnp.dot(a, b, precision=lax.Precision.HIGHEST, preferred_element_type=jnp.float32)

        iterate = hermit / frob
        inverse = identity
        for step in range(NSIT):
            factor = 1.5 * identity - 0.5 * (iterate if step == 0 else mul(inverse, iterate))
            if step < NSIT - 1:
                iterate = mul(iterate, factor)
                inverse = factor if step == 0 else mul(factor, inverse)
            else:
                inverse = mul(factor[:NB], inverse)
        scaled = inverse[:NB] * jnp.sqrt(6.0 * points / frob)
        msg[:16, :] = jnp.concatenate([scaled[:16], scaled[16:]], axis=1).astype(jnp.bfloat16)
        high = energy.astype(jnp.bfloat16).astype(jnp.float32)
        lane = lax.broadcasted_iota(jnp.int32, (16, 128), 1)
        tail = jnp.where(lane == 0, high, jnp.where(lane == 1, energy - high, 0.0))
        msg[16:, :] = tail.astype(jnp.bfloat16)
        crecv[mine] = msg[...]

        @pl.loop(1, total)
        def _(k):
            coef_to((lin + k) % total).start()

    for slot in range(slots):
        if shared[slot]:
            @pl.when(member(tm, shared[slot]))
            def _(slot=slot):
                for c in range(3):
                    exchange(slot, c).wait_send()

                @pl.loop(1, half_n)
                def _(k):
                    scatter(slot, same_side(k)).wait_send()

        if whole[slot]:
            @pl.when(member(tm, whole[slot]))
            def _(slot=slot):
                @pl.loop(1, half_n)
                def _(k):
                    scatter(slot, same_side(k)).wait_send()

                @pl.loop(0, half_n)
                def _(k):
                    scatter(slot, other_side(k)).wait_send()

    for f in range(NF):
        @pl.when(lin != owner(f))
        def _(f=f):
            to_owner(f).wait_send()

    for f in range(NF):
        @pl.when(lin != owner(f))
        def _(f=f):
            pltpu.make_async_remote_copy(
                src_ref=msg, dst_ref=crecv.at[f], send_sem=csend.at[f], recv_sem=crcv.at[f],
                device_id=where_is(owner(f)), device_id_type=MESH).wait_recv()

    lanes = lax.broadcasted_iota(jnp.int32, (NB, 2 * NB), 1)
    signs = jnp.where(lanes < NB, 1.0, -1.0).astype(jnp.bfloat16)
    wide_lane = lax.broadcasted_iota(jnp.int32, (1, NF), 1)
    energies = jnp.zeros((1, NF), jnp.float32)
    for f in range(NF):
        pairs = crecv[f, :16, :]
        straight = jnp.concatenate([pairs[:, : 2 * NB], pairs[:, 2 * NB :]], axis=0)
        crossed = jnp.concatenate([straight[:, NB:], straight[:, :NB]], axis=1)
        stacked = jnp.concatenate([straight * signs, crossed], axis=0)
        tiled = jnp.concatenate([stacked] * 3, axis=1)
        full = jnp.dot(spread_ref[...], tiled, preferred_element_type=jnp.float32)
        full = (full * mask_ref[...]).astype(jnp.bfloat16)
        modes_ref[f * 6 * NB : (f + 1) * 6 * NB, :] = jnp.dot(
            full, spec[f], preferred_element_type=jnp.float32).astype(jnp.bfloat16)
        tail = crecv[f, 16:, :].astype(jnp.float32)
        energies = jnp.where(wide_lane == f, jnp.sum(tail[:1, :], axis=1, keepdims=True), energies)
    energy_ref[...] = energies

    @pl.when(owns)
    def _():
        @pl.loop(1, total)
        def _(k):
            coef_to((lin + k) % total).wait_send()


def fused(n, nf_dev, chosen, snapshots, block_starts, freq_index):
    per, whole, shared, holders = chosen
    rows, count, wide = snapshots.shape
    total = n * nf_dev
    pw = wide // n
    slots = per + 4
    f32, bf16 = jnp.float32, jnp.bfloat16
    dma = pltpu.SemaphoreType.DMA
    vmem = pl.BlockSpec(memory_space=pltpu.VMEM)
    modes, energy = pl.pallas_call(
        functools.partial(kernel, n, nf_dev, per, whole, shared, holders, float(wide * nf_dev)),
        out_shape=(jax.ShapeDtypeStruct((NF * NB * 6, pw), bf16), jax.ShapeDtypeStruct((1, NF), f32)),
        in_specs=[pl.BlockSpec(memory_space=pltpu.HBM)] * 3,
        out_specs=(vmem, vmem),
        scratch_shapes=[
            pltpu.SMEM((NB,), jnp.int32),
            pltpu.SMEM((NF,), jnp.int32),
            pltpu.VMEM((slots * ROWS, rows), bf16),
            pltpu.VMEM((NB * 6, 2 * NB), bf16),
            pltpu.VMEM((NB * 6, 6 * NB), f32),
            pltpu.VMEM((3, rows, wide), bf16),
            pltpu.VMEM((slots, 2, 3, ROWS, wide // 2), f32),
            pltpu.VMEM((slots, 3, ROWS, wide // 2), f32),
            pltpu.VMEM((slots, n, ROWS, 3 * pw), bf16),
            pltpu.VMEM((NB, ROWS, 3 * pw), bf16),
            pltpu.VMEM((3, NB * ROWS, pw), f32),
            pltpu.VMEM((NF, 6 * NB, pw), bf16),
            pltpu.VMEM((NF, NB // 2, 4 * NB), f32),
            pltpu.VMEM((total, NB // 2, 4 * NB), f32),
            pltpu.VMEM((32, 4 * NB), bf16),
            pltpu.VMEM((NF, 32, 4 * NB), bf16),
            dma((5,)), dma((slots, 3)), dma((slots, 3)), dma((slots, n)), dma((NB,)),
            dma((NF,)), dma((total,)), dma((total,)), dma((NF,)),
        ],
        compiler_params=pltpu.CompilerParams(
            collective_id=0, has_side_effects=True, vmem_limit_bytes=64_500_000),
    )(jnp.transpose(snapshots, (1, 0, 2)), block_starts, freq_index)
    modes = modes.reshape(NF, NB, 3, 2, pw).transpose(0, 1, 3, 2, 4)
    return modes, energy.reshape(NF)


def solution(mesh):
    n, nf_dev = mesh.shape["tm"], mesh.shape["freq"]

    def body(snapshots, block_starts, freq_index):
        rows, _, wide = snapshots.shape
        chosen = plan(n, rows, n * nf_dev, wide // n)
        if chosen is None:
            return local(snapshots, block_starts, freq_index)
        return fused(n, nf_dev, chosen, snapshots, block_starts, freq_index)

    return jax.shard_map(
        body,
        mesh=mesh,
        in_specs=(P("tm", None, "freq"), P(), P()),
        out_specs=(P(None, None, None, None, ("freq", "tm")), P()),
        check_vma=False,
    )
```

```python
import functools
import math

import jax
import jax.numpy as jnp
import numpy as np
from jax import lax
from jax.experimental import pallas as pl
from jax.experimental.pallas import tpu as pltpu
from jax.sharding import PartitionSpec as P

NB = 32
NFFT = 256
NF = 16
NSIT = 6


def for_sending(shard):
    return jax.tree.map(lambda a: a.astype(jnp.bfloat16) if a.dtype == jnp.float32 else a, shard)


def dft_rows(freq_index):
    times_idx = jnp.arange(NFFT, dtype=jnp.int32)
    phase_int = freq_index[:, None] * times_idx[None, :] % NFFT
    angles = 2.0 * math.pi / NFFT * phase_int.astype(jnp.float32)
    window = 0.5 - 0.5 * jnp.cos(2.0 * math.pi / NFFT * times_idx.astype(jnp.float32))
    scaling = 1.0 / jnp.sqrt(jnp.sum(window * window))
    cosine = window[None, :] * jnp.cos(angles) * scaling
    sine_rows = -window[None, :] * jnp.sin(angles) * scaling
    return jnp.stack([cosine, sine_rows], 1).reshape(2 * NF, NFFT).astype(jnp.bfloat16)


def block_rows(block_starts):
    return block_starts[:, None] + jnp.arange(NFFT, dtype=jnp.int32)[None, :]


def matmul_batch(left, right):
    return jnp.einsum("fij,fjk->fik", left, right, precision=lax.Precision.HIGHEST)


def whiten(summed, points):
    gram_re = summed[:, 0]
    gram_im = summed[:, 1]
    top_rows = jnp.concatenate([gram_re, -gram_im], 2)
    low_rows = jnp.concatenate([gram_im, gram_re], 2)
    hermit = jnp.concatenate([top_rows, low_rows], 1)
    frob = jnp.sqrt(jnp.sum(hermit * hermit, axis=(1, 2)) + 1e-06)
    identity = jnp.eye(2 * NB, dtype=jnp.float32)[None]
    iterate = hermit / frob[:, None, None]
    inverse = jnp.broadcast_to(identity, hermit.shape)
    for iteration in range(NSIT):
        factor = 1.5 * identity - 0.5 * matmul_batch(inverse, iterate)
        iterate = matmul_batch(iterate, factor)
        inverse = matmul_batch(factor, inverse)
    columns = inverse[:, :, :NB] * jnp.sqrt(6.0 * points / frob)[:, None, None]
    upper = columns[:, :NB]
    lower = columns[:, NB:]
    coefficients = jnp.stack([jnp.stack([upper, -lower], 1), jnp.stack([lower, upper], 1)], 1)
    energy = jnp.trace(gram_re, axis1=1, axis2=2) / (3.0 * NB * points)
    return (coefficients, energy)


def local(snapshots, block_starts, freq_index):
    dft_table = dft_rows(freq_index)
    offsets = block_rows(block_starts)
    series = lax.all_to_all(snapshots, "tm", split_axis=2, concat_axis=0, tiled=True)
    count = series.shape[1]
    width = series.shape[2]
    columns_all = series.reshape(series.shape[0], count * width)
    windows = jnp.take(columns_all, offsets, axis=0)
    spectra_part = jnp.einsum(
        "rt,btn->rbn", dft_table, windows, preferred_element_type=jnp.float32
    ).astype(jnp.bfloat16)
    spectra = spectra_part.reshape(2 * NF, NB, count, width)
    width = spectra.shape[3]
    points = float(width * lax.axis_size("tm") * lax.axis_size("freq"))
    flat_spec = spectra.reshape(NF, 2, NB, 3 * width)
    real_part = flat_spec[:, 0]
    imag_part = flat_spec[:, 1]
    gram_re = jnp.einsum("fbn,fcn->fbc", real_part, real_part, preferred_element_type=jnp.float32)
    gram_re = gram_re + jnp.einsum(
        "fbn,fcn->fbc", imag_part, imag_part, preferred_element_type=jnp.float32
    )
    cross_terms = jnp.einsum(
        "fbn,fcn->fbc", real_part, imag_part, preferred_element_type=jnp.float32
    )
    partial_gram = jnp.stack([gram_re, cross_terms - jnp.swapaxes(cross_terms, 1, 2)], 1)
    shared = lax.psum_scatter(partial_gram, "freq", scatter_dimension=0, tiled=True)
    shared = lax.psum(shared, "tm")
    coef_part, energy_part = whiten(shared, points)
    coefficients, energy = (
        lax.all_gather(for_sending(coef_part), "freq", axis=0, tiled=True).astype(coef_part.dtype),
        lax.all_gather(for_sending(energy_part), "freq", axis=0, tiled=True).astype(
            energy_part.dtype
        ),
    )
    coef_bf = jnp.transpose(coefficients.astype(jnp.bfloat16), (0, 4, 1, 2, 3))
    modes = jnp.einsum(
        "fjorb,frbn->fjon", coef_bf, flat_spec, preferred_element_type=jnp.float32
    ).astype(jnp.bfloat16)
    return (modes.reshape(NF, NB, 2, 3, width), energy)


MESH = pl.DeviceIdType.MESH
ROWS = 2 * NF
HOP = 128
JIT = 64


def plan(n, rows, total, width):
    if n < 2 or n % 2 or NB % n or total % (2 * NF) or width != 128 or rows % 16:
        return None
    per = NB // n
    if per < 4 or per % 2:
        return None
    slots = per + 4
    whole = [[] for _ in range(slots)]
    shared = [[] for _ in range(slots)]
    holders = []
    for block in range(NB):
        touched = [
            dev for dev in range(n)
            if HOP * block < rows * (dev + 1) and HOP * block + JIT + NFFT > rows * dev
        ]
        holders.append(touched)
        if len(touched) > 2:
            return None
        for dev in touched:
            slot = block - per * dev + 2
            if not 0 <= slot < slots:
                return None
            if len(touched) == 2:
                if (slot < slots // 2) != (dev == touched[1]):
                    return None
                shared[slot].append(dev)
            else:
                whole[slot].append(dev)
    return per, whole, shared, holders


def base_table(freq_ref):
    row = lax.broadcasted_iota(jnp.int32, (ROWS, NFFT), 0)
    times_idx = lax.broadcasted_iota(jnp.int32, (ROWS, NFFT), 1)
    freqs = jnp.zeros((ROWS, NFFT), jnp.int32)
    for f in range(NF):
        freqs = jnp.where((row >> 1) == f, freq_ref[f], freqs)
    phase = (freqs * times_idx) & (NFFT - 1)
    angles = 2.0 * math.pi / NFFT * phase.astype(jnp.float32)
    window = 0.5 - 0.5 * jnp.cos(2.0 * math.pi / NFFT * times_idx.astype(jnp.float32))
    hann = 0.5 - 0.5 * np.cos(2.0 * math.pi / NFFT * np.arange(NFFT))
    scaling = np.float32(1.0 / np.sqrt(np.sum(hann * hann)))
    cosine = window * jnp.cos(angles) * scaling
    sine = -window * jnp.sin(angles) * scaling
    return jnp.where((row & 1) == 1, sine, cosine).astype(jnp.bfloat16)


def shifted(base, shift, rows):
    source = lax.broadcasted_iota(jnp.int32, (NFFT, rows), 0)
    target = lax.broadcasted_iota(jnp.int32, (NFFT, rows), 1)
    pick = jnp.where(source - target == shift, 1.0, 0.0).astype(jnp.bfloat16)
    return jnp.dot(base, pick, preferred_element_type=jnp.float32).astype(jnp.bfloat16)


def expanders(spread_ref, mask_ref):
    row = lax.broadcasted_iota(jnp.int32, (NB * 6, 2 * NB), 0)
    col = lax.broadcasted_iota(jnp.int32, (NB * 6, 2 * NB), 1)
    first = 6 * (col & (NB - 1))
    hit = (row >= first) & (row < first + 6) & ((row & 1) == jnp.where(col >= NB, 1, 0))
    spread_ref[...] = jnp.where(hit, 1.0, 0.0).astype(jnp.bfloat16)
    row = lax.broadcasted_iota(jnp.int32, (NB * 6, 6 * NB), 0)
    col = lax.broadcasted_iota(jnp.int32, (NB * 6, 6 * NB), 1)
    pair = row >> 1
    comp = pair - 3 * ((pair * 43691) >> 17)
    part = jnp.where(col >= 4 * NB, 2, jnp.where(col >= 2 * NB, 1, 0))
    mask_ref[...] = jnp.where(comp == part, 1.0, 0.0)


def member(index, devs):
    if not devs:
        return None
    if devs == list(range(devs[0], devs[-1] + 1)):
        return (index >= devs[0]) & (index <= devs[-1])
    hit = index == devs[0]
    for dev in devs[1:]:
        hit = hit | (index == dev)
    return hit


def kernel(n, nf_dev, per, whole, shared, holders, points, x_hbm, starts_hbm, freq_hbm,
           modes_ref, energy_ref, starts_ref, freq_ref, t_ref, spread_ref, mask_ref, xv, parts,
           others, sendb, recvb, spec32, spec, gpart, gath, msg, crecv, load_sem, psend, precv,
           asend, arecv, gsend, grecv, csend, crcv):
    tm = lax.axis_index("tm")
    fr = lax.axis_index("freq")
    total = n * nf_dev
    lin = tm * nf_dev + fr
    step, lowest = total // (2 * NF), total // 4
    slots = per + 4
    mine = (lin - lowest) // step
    owns = (lin >= lowest) & (lin < lowest + NF * step) & ((lin - lowest) % step == 0)
    half_n = n // 2
    parity = tm % 2

    def owner(f):
        return lowest + f * step

    def where_is(index):
        return {"tm": index // nf_dev, "freq": index % nf_dev}

    small = [
        pltpu.make_async_copy(starts_hbm, starts_ref, load_sem.at[3]),
        pltpu.make_async_copy(freq_hbm, freq_ref, load_sem.at[4]),
    ]
    for copy in small:
        copy.start()
    for c in range(3):
        pltpu.make_async_copy(x_hbm.at[c], xv.at[c], load_sem.at[c]).start()
    barrier = pltpu.get_barrier_semaphore()

    @pl.loop(1, total)
    def _(k):
        pl.semaphore_signal(barrier, inc=1, device_id=where_is((lin + k) % total), device_id_type=MESH)

    for copy in small:
        copy.wait()
    rows = xv.shape[1]
    base = base_table(freq_ref)
    for slot in range(slots):
        block = per * tm + slot - 2
        start = starts_ref[jnp.clip(block, 0, NB - 1)]
        inside = (block >= 0) & (block < NB)
        shift = jnp.where(inside, rows * tm - start, 4 * (rows + NFFT))
        t_ref[slot * ROWS : (slot + 1) * ROWS, :] = shifted(base, shift, rows)
    expanders(spread_ref, mask_ref)
    width = xv.shape[2]
    pw = width // n
    def exchange(slot):
        low = slot < slots // 2
        there = slot + per if low else slot - per
        return pltpu.make_async_remote_copy(
            src_ref=parts.at[slot, 1 - parity], dst_ref=others.at[there],
            send_sem=psend.at[slot], recv_sem=precv.at[there],
            device_id={"tm": (tm + n - 1) % n if low else (tm + 1) % n, "freq": fr},
            device_id_type=MESH)

    def arrival(slot):
        return pltpu.make_async_remote_copy(
            src_ref=parts.at[slot, 1 - parity], dst_ref=others.at[slot],
            send_sem=psend.at[slot], recv_sem=precv.at[slot],
            device_id={"tm": tm, "freq": fr}, device_id_type=MESH)

    outward = []
    for reach in range(slots // 2):
        outward += [slots // 2 + reach, slots // 2 - 1 - reach]
    inward = [slot + per if slot < slots // 2 else slot - per for slot in outward]

    for c in range(3):
        pltpu.make_async_copy(x_hbm.at[c], xv.at[c], load_sem.at[c]).wait()
        part = jnp.dot(t_ref[...], xv[c], preferred_element_type=jnp.float32)
        for slot in range(slots):
            for dest in range(n):
                at = dest // 2 * pw
                parts[slot, dest % 2, c, :, at : at + pw] = part[
                    slot * ROWS : (slot + 1) * ROWS, dest * pw : (dest + 1) * pw]
    pl.semaphore_wait(barrier, total - 1)

    for slot in outward:
        if shared[slot]:
            @pl.when(member(tm, shared[slot]))
            def _(slot=slot):
                exchange(slot).start()

    def scatter(slot, dest):
        return pltpu.make_async_remote_copy(
            src_ref=sendb.at[slot, dest], dst_ref=recvb.at[per * tm + slot - 2],
            send_sem=asend.at[slot, dest], recv_sem=arecv.at[per * tm + slot - 2],
            device_id={"tm": dest, "freq": fr}, device_id_type=MESH)

    def same_side(k):
        return 2 * ((tm // 2 + k) % half_n) + parity

    def other_side(k):
        return 2 * ((tm // 2 + k) % half_n) + 1 - parity

    def finish(slot, side, add):
        for q in range(half_n):
            for c in range(3):
                at = q * pw
                value = parts[slot, side, c, :, at : at + pw]
                if add:
                    value = value + others[slot, c, :, at : at + pw]
                sendb[slot, 2 * q + side, :, c * pw : (c + 1) * pw] = value.astype(jnp.bfloat16)

    def keep(slot):
        recvb[per * tm + slot - 2] = sendb[slot, tm]

    for slot in range(slots):
        if whole[slot]:
            @pl.when(member(tm, whole[slot]))
            def _(slot=slot):
                finish(slot, parity, False)
                finish(slot, 1 - parity, False)

                @pl.loop(1, half_n)
                def _(k):
                    scatter(slot, same_side(k)).start()

                @pl.loop(0, half_n)
                def _(k):
                    scatter(slot, other_side(k)).start()

                keep(slot)

    for slot in inward:
        if shared[slot]:
            @pl.when(member(tm, shared[slot]))
            def _(slot=slot):
                arrival(slot).wait_recv()
                finish(slot, parity, True)

                @pl.loop(1, half_n)
                def _(k):
                    scatter(slot, same_side(k)).start()

                keep(slot)

    ordered = [b for b in range(NB) if len(holders[b]) == 1] + [b for b in range(NB) if len(holders[b]) == 2]
    for block in ordered:
        @pl.when(jnp.logical_not(member(tm, holders[block])))
        def _(block=block):
            pltpu.make_async_remote_copy(
                src_ref=sendb.at[0, 0], dst_ref=recvb.at[block], send_sem=asend.at[0, 0],
                recv_sem=arecv.at[block], device_id={"tm": tm, "freq": fr},
                device_id_type=MESH).wait_recv()

    for block in range(NB):
        values = recvb[block]
        for c in range(3):
            spec32[c, block * ROWS : (block + 1) * ROWS, :] = values[:, c * 128 : (c + 1) * 128].astype(jnp.float32)

    def to_owner(f):
        return pltpu.make_async_remote_copy(
            src_ref=gpart.at[f], dst_ref=gath.at[lin], send_sem=gsend.at[f],
            recv_sem=grecv.at[lin], device_id=where_is(owner(f)), device_id_type=MESH)

    for f in range(NF):
        real = [spec32[c, pl.ds(2 * f, NB, stride=ROWS), :].astype(jnp.bfloat16) for c in range(3)]
        imag = [spec32[c, pl.ds(2 * f + 1, NB, stride=ROWS), :].astype(jnp.bfloat16) for c in range(3)]
        for c in range(3):
            spec[f, c * 2 * NB : c * 2 * NB + NB, :] = real[c]
            spec[f, c * 2 * NB + NB : (c + 1) * 2 * NB, :] = imag[c]
        lhs = jnp.concatenate(real + imag, axis=1)
        rhs = jnp.concatenate([lhs, jnp.concatenate(imag + [-v for v in real], axis=1)], axis=0)
        gram = lax.dot_general(lhs, rhs, (((1,), (1,)), ((), ())), preferred_element_type=jnp.float32)
        half = NB // 2
        gpart[f] = jnp.concatenate([gram[:half], gram[half:]], axis=1)
        if f % 4 == 3:
            for sent in range(f - 3, f + 1):
                @pl.when(lin != owner(sent))
                def _(sent=sent):
                    to_owner(sent).start()

    def coef_to(index):
        return pltpu.make_async_remote_copy(
            src_ref=msg, dst_ref=crecv.at[mine], send_sem=csend.at[index],
            recv_sem=crcv.at[mine], device_id=where_is(index), device_id_type=MESH)

    @pl.when(owns)
    def _():
        gath[lin] = gpart[mine]

        @pl.loop(1, total)
        def _(k):
            src = (lin + k) % total
            pltpu.make_async_remote_copy(
                src_ref=gpart.at[0], dst_ref=gath.at[src], send_sem=gsend.at[0],
                recv_sem=grecv.at[src], device_id=where_is(src), device_id_type=MESH).wait_recv()

        packed = jnp.sum(gath[...], axis=0)
        both = jnp.concatenate([packed[:, : 2 * NB], packed[:, 2 * NB :]], axis=0)
        gram_re = both[:, :NB]
        gram_im = both[:, NB:]
        hermit = jnp.concatenate([
            jnp.concatenate([gram_re, -gram_im], axis=1),
            jnp.concatenate([gram_im, gram_re], axis=1)], axis=0)
        frob = jnp.sqrt(jnp.sum(hermit * hermit, axis=(0, 1), keepdims=True) + 1e-06)
        ri = lax.broadcasted_iota(jnp.int32, (2 * NB, 2 * NB), 0)
        ci = lax.broadcasted_iota(jnp.int32, (2 * NB, 2 * NB), 1)
        identity = jnp.where(ri == ci, 1.0, 0.0).astype(jnp.float32)
        energy = jnp.sum(jnp.where((ri == ci) & (ri < NB), hermit, 0.0), axis=(0, 1), keepdims=True) / (3.0 * NB * points)

        def mul(a, b):
            return jnp.dot(a, b, precision=lax.Precision.HIGHEST, preferred_element_type=jnp.float32)

        iterate = hermit / frob
        inverse = identity
        for step in range(NSIT):
            factor = 1.5 * identity - 0.5 * (iterate if step == 0 else mul(inverse, iterate))
            if step < NSIT - 1:
                iterate = mul(iterate, factor)
                inverse = factor if step == 0 else mul(factor, inverse)
            else:
                inverse = mul(factor[:NB], inverse)
        scaled = inverse[:NB] * jnp.sqrt(6.0 * points / frob)
        msg[:16, :] = jnp.concatenate([scaled[:16], scaled[16:]], axis=1).astype(jnp.bfloat16)
        high = energy.astype(jnp.bfloat16).astype(jnp.float32)
        lane = lax.broadcasted_iota(jnp.int32, (16, 128), 1)
        tail = jnp.where(lane == 0, high, jnp.where(lane == 1, energy - high, 0.0))
        msg[16:, :] = tail.astype(jnp.bfloat16)
        crecv[mine] = msg[...]

        @pl.loop(1, total)
        def _(k):
            coef_to((lin + k) % total).start()

    for slot in range(slots):
        if shared[slot]:
            @pl.when(member(tm, shared[slot]))
            def _(slot=slot):
                exchange(slot).wait_send()

                @pl.loop(1, half_n)
                def _(k):
                    scatter(slot, same_side(k)).wait_send()

        if whole[slot]:
            @pl.when(member(tm, whole[slot]))
            def _(slot=slot):
                @pl.loop(1, half_n)
                def _(k):
                    scatter(slot, same_side(k)).wait_send()

                @pl.loop(0, half_n)
                def _(k):
                    scatter(slot, other_side(k)).wait_send()

    for f in range(NF):
        @pl.when(lin != owner(f))
        def _(f=f):
            to_owner(f).wait_send()

    for f in range(NF):
        @pl.when(lin != owner(f))
        def _(f=f):
            pltpu.make_async_remote_copy(
                src_ref=msg, dst_ref=crecv.at[f], send_sem=csend.at[f], recv_sem=crcv.at[f],
                device_id=where_is(owner(f)), device_id_type=MESH).wait_recv()

    lanes = lax.broadcasted_iota(jnp.int32, (NB, 2 * NB), 1)
    signs = jnp.where(lanes < NB, 1.0, -1.0).astype(jnp.bfloat16)
    wide_lane = lax.broadcasted_iota(jnp.int32, (1, NF), 1)
    energies = jnp.zeros((1, NF), jnp.float32)
    for f in range(NF):
        pairs = crecv[f, :16, :]
        straight = jnp.concatenate([pairs[:, : 2 * NB], pairs[:, 2 * NB :]], axis=0)
        crossed = jnp.concatenate([straight[:, NB:], straight[:, :NB]], axis=1)
        stacked = jnp.concatenate([straight * signs, crossed], axis=0)
        tiled = jnp.concatenate([stacked] * 3, axis=1)
        full = jnp.dot(spread_ref[...], tiled, preferred_element_type=jnp.float32)
        full = (full * mask_ref[...]).astype(jnp.bfloat16)
        modes_ref[f * 6 * NB : (f + 1) * 6 * NB, :] = jnp.dot(
            full, spec[f], preferred_element_type=jnp.float32).astype(jnp.bfloat16)
        tail = crecv[f, 16:, :].astype(jnp.float32)
        energies = jnp.where(wide_lane == f, jnp.sum(tail[:1, :], axis=1, keepdims=True), energies)
    energy_ref[...] = energies

    @pl.when(owns)
    def _():
        @pl.loop(1, total)
        def _(k):
            coef_to((lin + k) % total).wait_send()


def fused(n, nf_dev, chosen, snapshots, block_starts, freq_index):
    per, whole, shared, holders = chosen
    rows, count, wide = snapshots.shape
    total = n * nf_dev
    pw = wide // n
    slots = per + 4
    f32, bf16 = jnp.float32, jnp.bfloat16
    dma = pltpu.SemaphoreType.DMA
    vmem = pl.BlockSpec(memory_space=pltpu.VMEM)
    modes, energy = pl.pallas_call(
        functools.partial(kernel, n, nf_dev, per, whole, shared, holders, float(wide * nf_dev)),
        out_shape=(jax.ShapeDtypeStruct((NF * NB * 6, pw), bf16), jax.ShapeDtypeStruct((1, NF), f32)),
        in_specs=[pl.BlockSpec(memory_space=pltpu.HBM)] * 3,
        out_specs=(vmem, vmem),
        scratch_shapes=[
            pltpu.SMEM((NB,), jnp.int32),
            pltpu.SMEM((NF,), jnp.int32),
            pltpu.VMEM((slots * ROWS, rows), bf16),
            pltpu.VMEM((NB * 6, 2 * NB), bf16),
            pltpu.VMEM((NB * 6, 6 * NB), f32),
            pltpu.VMEM((3, rows, wide), bf16),
            pltpu.VMEM((slots, 2, 3, ROWS, wide // 2), f32),
            pltpu.VMEM((slots, 3, ROWS, wide // 2), f32),
            pltpu.VMEM((slots, n, ROWS, 3 * pw), bf16),
            pltpu.VMEM((NB, ROWS, 3 * pw), bf16),
            pltpu.VMEM((3, NB * ROWS, pw), f32),
            pltpu.VMEM((NF, 6 * NB, pw), bf16),
            pltpu.VMEM((NF, NB // 2, 4 * NB), f32),
            pltpu.VMEM((total, NB // 2, 4 * NB), f32),
            pltpu.VMEM((32, 4 * NB), bf16),
            pltpu.VMEM((NF, 32, 4 * NB), bf16),
            dma((5,)), dma((slots,)), dma((slots,)), dma((slots, n)), dma((NB,)),
            dma((NF,)), dma((total,)), dma((total,)), dma((NF,)),
        ],
        compiler_params=pltpu.CompilerParams(
            collective_id=0, has_side_effects=True, vmem_limit_bytes=54_000_000),
    )(jnp.transpose(snapshots, (1, 0, 2)), block_starts, freq_index)
    modes = modes.reshape(NF, NB, 3, 2, pw).transpose(0, 1, 3, 2, 4)
    return modes, energy.reshape(NF)


def solution(mesh):
    n, nf_dev = mesh.shape["tm"], mesh.shape["freq"]

    def body(snapshots, block_starts, freq_index):
        rows, _, wide = snapshots.shape
        chosen = plan(n, rows, n * nf_dev, wide // n)
        if chosen is None:
            return local(snapshots, block_starts, freq_index)
        return fused(n, nf_dev, chosen, snapshots, block_starts, freq_index)

    return jax.shard_map(
        body,
        mesh=mesh,
        in_specs=(P("tm", None, "freq"), P(), P()),
        out_specs=(P(None, None, None, None, ("freq", "tm")), P()),
        check_vma=False,
    )
```

```python
import functools
import math

import jax
import jax.numpy as jnp
import numpy as np
from jax import lax
from jax.experimental import pallas as pl
from jax.experimental.pallas import tpu as pltpu
from jax.sharding import PartitionSpec as P

NB = 32
NFFT = 256
NF = 16
NSIT = 6


def for_sending(shard):
    return jax.tree.map(lambda a: a.astype(jnp.bfloat16) if a.dtype == jnp.float32 else a, shard)


def dft_rows(freq_index):
    times_idx = jnp.arange(NFFT, dtype=jnp.int32)
    phase_int = freq_index[:, None] * times_idx[None, :] % NFFT
    angles = 2.0 * math.pi / NFFT * phase_int.astype(jnp.float32)
    window = 0.5 - 0.5 * jnp.cos(2.0 * math.pi / NFFT * times_idx.astype(jnp.float32))
    scaling = 1.0 / jnp.sqrt(jnp.sum(window * window))
    cosine = window[None, :] * jnp.cos(angles) * scaling
    sine_rows = -window[None, :] * jnp.sin(angles) * scaling
    return jnp.stack([cosine, sine_rows], 1).reshape(2 * NF, NFFT).astype(jnp.bfloat16)


def block_rows(block_starts):
    return block_starts[:, None] + jnp.arange(NFFT, dtype=jnp.int32)[None, :]


def matmul_batch(left, right):
    return jnp.einsum("fij,fjk->fik", left, right, precision=lax.Precision.HIGHEST)


def whiten(summed, points):
    gram_re = summed[:, 0]
    gram_im = summed[:, 1]
    top_rows = jnp.concatenate([gram_re, -gram_im], 2)
    low_rows = jnp.concatenate([gram_im, gram_re], 2)
    hermit = jnp.concatenate([top_rows, low_rows], 1)
    frob = jnp.sqrt(jnp.sum(hermit * hermit, axis=(1, 2)) + 1e-06)
    identity = jnp.eye(2 * NB, dtype=jnp.float32)[None]
    iterate = hermit / frob[:, None, None]
    inverse = jnp.broadcast_to(identity, hermit.shape)
    for iteration in range(NSIT):
        factor = 1.5 * identity - 0.5 * matmul_batch(inverse, iterate)
        iterate = matmul_batch(iterate, factor)
        inverse = matmul_batch(factor, inverse)
    columns = inverse[:, :, :NB] * jnp.sqrt(6.0 * points / frob)[:, None, None]
    upper = columns[:, :NB]
    lower = columns[:, NB:]
    coefficients = jnp.stack([jnp.stack([upper, -lower], 1), jnp.stack([lower, upper], 1)], 1)
    energy = jnp.trace(gram_re, axis1=1, axis2=2) / (3.0 * NB * points)
    return (coefficients, energy)


def local(snapshots, block_starts, freq_index):
    dft_table = dft_rows(freq_index)
    offsets = block_rows(block_starts)
    series = lax.all_to_all(snapshots, "tm", split_axis=2, concat_axis=0, tiled=True)
    count = series.shape[1]
    width = series.shape[2]
    columns_all = series.reshape(series.shape[0], count * width)
    windows = jnp.take(columns_all, offsets, axis=0)
    spectra_part = jnp.einsum(
        "rt,btn->rbn", dft_table, windows, preferred_element_type=jnp.float32
    ).astype(jnp.bfloat16)
    spectra = spectra_part.reshape(2 * NF, NB, count, width)
    width = spectra.shape[3]
    points = float(width * lax.axis_size("tm") * lax.axis_size("freq"))
    flat_spec = spectra.reshape(NF, 2, NB, 3 * width)
    real_part = flat_spec[:, 0]
    imag_part = flat_spec[:, 1]
    gram_re = jnp.einsum("fbn,fcn->fbc", real_part, real_part, preferred_element_type=jnp.float32)
    gram_re = gram_re + jnp.einsum(
        "fbn,fcn->fbc", imag_part, imag_part, preferred_element_type=jnp.float32
    )
    cross_terms = jnp.einsum(
        "fbn,fcn->fbc", real_part, imag_part, preferred_element_type=jnp.float32
    )
    partial_gram = jnp.stack([gram_re, cross_terms - jnp.swapaxes(cross_terms, 1, 2)], 1)
    shared = lax.psum_scatter(partial_gram, "freq", scatter_dimension=0, tiled=True)
    shared = lax.psum(shared, "tm")
    coef_part, energy_part = whiten(shared, points)
    coefficients, energy = (
        lax.all_gather(for_sending(coef_part), "freq", axis=0, tiled=True).astype(coef_part.dtype),
        lax.all_gather(for_sending(energy_part), "freq", axis=0, tiled=True).astype(
            energy_part.dtype
        ),
    )
    coef_bf = jnp.transpose(coefficients.astype(jnp.bfloat16), (0, 4, 1, 2, 3))
    modes = jnp.einsum(
        "fjorb,frbn->fjon", coef_bf, flat_spec, preferred_element_type=jnp.float32
    ).astype(jnp.bfloat16)
    return (modes.reshape(NF, NB, 2, 3, width), energy)


MESH = pl.DeviceIdType.MESH
ROWS = 2 * NF
HOP = 128
JIT = 64


def plan(n, rows, total, width):
    if n < 2 or n % 2 or NB % n or total % (2 * NF) or width != 128 or rows % 16:
        return None
    per = NB // n
    if per < 4 or per % 2:
        return None
    slots = per + 4
    whole = [[] for _ in range(slots)]
    shared = [[] for _ in range(slots)]
    holders = []
    for block in range(NB):
        touched = [
            dev for dev in range(n)
            if HOP * block < rows * (dev + 1) and HOP * block + JIT + NFFT > rows * dev
        ]
        holders.append(touched)
        if len(touched) > 2:
            return None
        for dev in touched:
            slot = block - per * dev + 2
            if not 0 <= slot < slots:
                return None
            if len(touched) == 2:
                if (slot < slots // 2) != (dev == touched[1]):
                    return None
                shared[slot].append(dev)
            else:
                whole[slot].append(dev)
    return per, whole, shared, holders


def base_table(ints_ref):
    row = lax.broadcasted_iota(jnp.int32, (ROWS, NFFT), 0)
    times_idx = lax.broadcasted_iota(jnp.int32, (ROWS, NFFT), 1)
    freqs = jnp.zeros((ROWS, NFFT), jnp.int32)
    for f in range(NF):
        freqs = jnp.where((row >> 1) == f, ints_ref[NB + f], freqs)
    phase = (freqs * times_idx) & (NFFT - 1)
    angles = 2.0 * math.pi / NFFT * phase.astype(jnp.float32)
    window = 0.5 - 0.5 * jnp.cos(2.0 * math.pi / NFFT * times_idx.astype(jnp.float32))
    hann = 0.5 - 0.5 * np.cos(2.0 * math.pi / NFFT * np.arange(NFFT))
    scaling = np.float32(1.0 / np.sqrt(np.sum(hann * hann)))
    cosine = window * jnp.cos(angles) * scaling
    sine = -window * jnp.sin(angles) * scaling
    return jnp.where((row & 1) == 1, sine, cosine).astype(jnp.bfloat16)


def shifted(base, shift, rows):
    source = lax.broadcasted_iota(jnp.int32, (NFFT, rows), 0)
    target = lax.broadcasted_iota(jnp.int32, (NFFT, rows), 1)
    pick = jnp.where(source - target == shift, 1.0, 0.0).astype(jnp.bfloat16)
    return jnp.dot(base, pick, preferred_element_type=jnp.float32).astype(jnp.bfloat16)


def expanders(spread_ref, mask_ref):
    row = lax.broadcasted_iota(jnp.int32, (NB * 6, 2 * NB), 0)
    col = lax.broadcasted_iota(jnp.int32, (NB * 6, 2 * NB), 1)
    first = 6 * (col & (NB - 1))
    hit = (row >= first) & (row < first + 6) & ((row & 1) == jnp.where(col >= NB, 1, 0))
    spread_ref[...] = jnp.where(hit, 1.0, 0.0).astype(jnp.bfloat16)
    row = lax.broadcasted_iota(jnp.int32, (NB * 6, 6 * NB), 0)
    col = lax.broadcasted_iota(jnp.int32, (NB * 6, 6 * NB), 1)
    pair = row >> 1
    comp = pair - 3 * ((pair * 43691) >> 17)
    part = jnp.where(col >= 4 * NB, 2, jnp.where(col >= 2 * NB, 1, 0))
    mask_ref[...] = jnp.where(comp == part, 1.0, 0.0)


def member(index, devs):
    if not devs:
        return None
    if devs == list(range(devs[0], devs[-1] + 1)):
        return (index >= devs[0]) & (index <= devs[-1])
    hit = index == devs[0]
    for dev in devs[1:]:
        hit = hit | (index == dev)
    return hit


def kernel(n, nf_dev, per, whole, shared, holders, points, x_hbm, ints_hbm,
           modes_ref, energy_ref, ints_ref, t_ref, spread_ref, mask_ref, xv, parts,
           others, sendb, recvb, spec32, spec, gpart, gath, msg, crecv, load_sem, psend, precv,
           asend, arecv, gsend, grecv, csend, crcv):
    tm = lax.axis_index("tm")
    fr = lax.axis_index("freq")
    total = n * nf_dev
    lin = tm * nf_dev + fr
    step, lowest = total // (2 * NF), total // 4
    slots = per + 4
    mine = (lin - lowest) // step
    owns = (lin >= lowest) & (lin < lowest + NF * step) & ((lin - lowest) % step == 0)
    half_n = n // 2
    parity = tm % 2

    def owner(f):
        return lowest + f * step

    def where_is(index):
        return {"tm": index // nf_dev, "freq": index % nf_dev}

    small = pltpu.make_async_copy(ints_hbm, ints_ref, load_sem.at[3])
    small.start()
    for c in range(3):
        pltpu.make_async_copy(x_hbm.at[c], xv.at[c], load_sem.at[c]).start()
    barrier = pltpu.get_barrier_semaphore()

    @pl.loop(1, total)
    def _(k):
        pl.semaphore_signal(barrier, inc=1, device_id=where_is((lin + k) % total), device_id_type=MESH)

    small.wait()
    rows = xv.shape[1]
    base = base_table(ints_ref)
    for slot in range(slots):
        block = per * tm + slot - 2
        start = ints_ref[jnp.clip(block, 0, NB - 1)]
        inside = (block >= 0) & (block < NB)
        shift = jnp.where(inside, rows * tm - start, 4 * (rows + NFFT))
        t_ref[slot * ROWS : (slot + 1) * ROWS, :] = shifted(base, shift, rows)
    expanders(spread_ref, mask_ref)
    width = xv.shape[2]
    pw = width // n
    def exchange(slot):
        low = slot < slots // 2
        there = slot + per if low else slot - per
        return pltpu.make_async_remote_copy(
            src_ref=parts.at[slot, 1 - parity], dst_ref=others.at[there],
            send_sem=psend.at[slot], recv_sem=precv.at[there],
            device_id={"tm": (tm + n - 1) % n if low else (tm + 1) % n, "freq": fr},
            device_id_type=MESH)

    def arrival(slot):
        return pltpu.make_async_remote_copy(
            src_ref=parts.at[slot, 1 - parity], dst_ref=others.at[slot],
            send_sem=psend.at[slot], recv_sem=precv.at[slot],
            device_id={"tm": tm, "freq": fr}, device_id_type=MESH)

    outward = []
    for reach in range(slots // 2):
        outward += [slots // 2 + reach, slots // 2 - 1 - reach]
    inward = [slot + per if slot < slots // 2 else slot - per for slot in outward]

    def compute(first, last):
        for c in range(3):
            part = jnp.dot(t_ref[first * ROWS : last * ROWS, :], xv[c], preferred_element_type=jnp.float32)
            for slot in range(first, last):
                for dest in range(n):
                    at = dest // 2 * pw
                    parts[slot, dest % 2, c, :, at : at + pw] = part[
                        (slot - first) * ROWS : (slot - first + 1) * ROWS, dest * pw : (dest + 1) * pw]

    def send_parts(chosen):
        for slot in chosen:
            if shared[slot]:
                @pl.when(member(tm, shared[slot]))
                def _(slot=slot):
                    exchange(slot).start()

    for c in range(3):
        pltpu.make_async_copy(x_hbm.at[c], xv.at[c], load_sem.at[c]).wait()
    inner = [slot for slot in outward if 2 <= slot < slots - 2]
    compute(2, slots - 2)
    pl.semaphore_wait(barrier, total - 1)
    send_parts(inner)
    compute(0, 2)
    compute(slots - 2, slots)
    send_parts([slot for slot in outward if slot not in inner])

    def scatter(slot, dest):
        return pltpu.make_async_remote_copy(
            src_ref=sendb.at[slot, dest], dst_ref=recvb.at[per * tm + slot - 2],
            send_sem=asend.at[slot, dest], recv_sem=arecv.at[per * tm + slot - 2],
            device_id={"tm": dest, "freq": fr}, device_id_type=MESH)

    def same_side(k):
        return 2 * ((tm // 2 + k) % half_n) + parity

    def other_side(k):
        return 2 * ((tm // 2 + k) % half_n) + 1 - parity

    def finish(slot, side, add):
        for q in range(half_n):
            for c in range(3):
                at = q * pw
                value = parts[slot, side, c, :, at : at + pw]
                if add:
                    value = value + others[slot, c, :, at : at + pw]
                sendb[slot, 2 * q + side, :, c * pw : (c + 1) * pw] = value.astype(jnp.bfloat16)

    def keep(slot):
        recvb[per * tm + slot - 2] = sendb[slot, tm]

    for slot in range(slots):
        if whole[slot]:
            @pl.when(member(tm, whole[slot]))
            def _(slot=slot):
                finish(slot, parity, False)
                finish(slot, 1 - parity, False)

                @pl.loop(1, half_n)
                def _(k):
                    scatter(slot, same_side(k)).start()

                @pl.loop(0, half_n)
                def _(k):
                    scatter(slot, other_side(k)).start()

                keep(slot)

    for slot in inward:
        if shared[slot]:
            @pl.when(member(tm, shared[slot]))
            def _(slot=slot):
                arrival(slot).wait_recv()
                finish(slot, parity, True)

                @pl.loop(1, half_n)
                def _(k):
                    scatter(slot, same_side(k)).start()

                keep(slot)

    ordered = [b for b in range(NB) if len(holders[b]) == 1] + [b for b in range(NB) if len(holders[b]) == 2]
    for block in ordered:
        @pl.when(jnp.logical_not(member(tm, holders[block])))
        def _(block=block):
            pltpu.make_async_remote_copy(
                src_ref=sendb.at[0, 0], dst_ref=recvb.at[block], send_sem=asend.at[0, 0],
                recv_sem=arecv.at[block], device_id={"tm": tm, "freq": fr},
                device_id_type=MESH).wait_recv()

    for block in range(NB):
        values = recvb[block]
        for c in range(3):
            spec32[c, block * ROWS : (block + 1) * ROWS, :] = values[:, c * 128 : (c + 1) * 128].astype(jnp.float32)

    def to_owner(f):
        return pltpu.make_async_remote_copy(
            src_ref=gpart.at[f], dst_ref=gath.at[lin], send_sem=gsend.at[f],
            recv_sem=grecv.at[lin], device_id=where_is(owner(f)), device_id_type=MESH)

    for f in range(NF):
        real = [spec32[c, pl.ds(2 * f, NB, stride=ROWS), :].astype(jnp.bfloat16) for c in range(3)]
        imag = [spec32[c, pl.ds(2 * f + 1, NB, stride=ROWS), :].astype(jnp.bfloat16) for c in range(3)]
        for c in range(3):
            spec[f, c * 2 * NB : c * 2 * NB + NB, :] = real[c]
            spec[f, c * 2 * NB + NB : (c + 1) * 2 * NB, :] = imag[c]
        lhs = jnp.concatenate(real + imag, axis=1)
        rhs = jnp.concatenate([lhs, jnp.concatenate(imag + [-v for v in real], axis=1)], axis=0)
        gram = lax.dot_general(lhs, rhs, (((1,), (1,)), ((), ())), preferred_element_type=jnp.float32)
        half = NB // 2
        gpart[f] = jnp.concatenate([gram[:half], gram[half:]], axis=1)
        if f % 4 == 3:
            for sent in range(f - 3, f + 1):
                @pl.when(lin != owner(sent))
                def _(sent=sent):
                    to_owner(sent).start()

    def coef_to(index):
        return pltpu.make_async_remote_copy(
            src_ref=msg, dst_ref=crecv.at[mine], send_sem=csend.at[index],
            recv_sem=crcv.at[mine], device_id=where_is(index), device_id_type=MESH)

    @pl.when(owns)
    def _():
        gath[lin] = gpart[mine]

        @pl.loop(1, total)
        def _(k):
            src = (lin + k) % total
            pltpu.make_async_remote_copy(
                src_ref=gpart.at[0], dst_ref=gath.at[src], send_sem=gsend.at[0],
                recv_sem=grecv.at[src], device_id=where_is(src), device_id_type=MESH).wait_recv()

        packed = jnp.sum(gath[...], axis=0)
        both = jnp.concatenate([packed[:, : 2 * NB], packed[:, 2 * NB :]], axis=0)
        gram_re = both[:, :NB]
        gram_im = both[:, NB:]
        hermit = jnp.concatenate([
            jnp.concatenate([gram_re, -gram_im], axis=1),
            jnp.concatenate([gram_im, gram_re], axis=1)], axis=0)
        frob = jnp.sqrt(jnp.sum(hermit * hermit, axis=(0, 1), keepdims=True) + 1e-06)
        ri = lax.broadcasted_iota(jnp.int32, (2 * NB, 2 * NB), 0)
        ci = lax.broadcasted_iota(jnp.int32, (2 * NB, 2 * NB), 1)
        identity = jnp.where(ri == ci, 1.0, 0.0).astype(jnp.float32)
        energy = jnp.sum(jnp.where((ri == ci) & (ri < NB), hermit, 0.0), axis=(0, 1), keepdims=True) / (3.0 * NB * points)

        def mul(a, b):
            return jnp.dot(a, b, precision=lax.Precision.HIGHEST, preferred_element_type=jnp.float32)

        iterate = hermit / frob
        inverse = identity
        for step in range(NSIT):
            factor = 1.5 * identity - 0.5 * (iterate if step == 0 else mul(inverse, iterate))
            if step < NSIT - 1:
                iterate = mul(iterate, factor)
                inverse = factor if step == 0 else mul(factor, inverse)
            else:
                inverse = mul(factor[:NB], inverse)
        scaled = inverse[:NB] * jnp.sqrt(6.0 * points / frob)
        msg[:16, :] = jnp.concatenate([scaled[:16], scaled[16:]], axis=1).astype(jnp.bfloat16)
        high = energy.astype(jnp.bfloat16).astype(jnp.float32)
        lane = lax.broadcasted_iota(jnp.int32, (16, 128), 1)
        tail = jnp.where(lane == 0, high, jnp.where(lane == 1, energy - high, 0.0))
        msg[16:, :] = tail.astype(jnp.bfloat16)
        crecv[mine] = msg[...]

        @pl.loop(1, total)
        def _(k):
            coef_to((lin + k) % total).start()

    for slot in range(slots):
        if shared[slot]:
            @pl.when(member(tm, shared[slot]))
            def _(slot=slot):
                exchange(slot).wait_send()

                @pl.loop(1, half_n)
                def _(k):
                    scatter(slot, same_side(k)).wait_send()

        if whole[slot]:
            @pl.when(member(tm, whole[slot]))
            def _(slot=slot):
                @pl.loop(1, half_n)
                def _(k):
                    scatter(slot, same_side(k)).wait_send()

                @pl.loop(0, half_n)
                def _(k):
                    scatter(slot, other_side(k)).wait_send()

    for f in range(NF):
        @pl.when(lin != owner(f))
        def _(f=f):
            to_owner(f).wait_send()

    for f in range(NF):
        @pl.when(lin != owner(f))
        def _(f=f):
            pltpu.make_async_remote_copy(
                src_ref=msg, dst_ref=crecv.at[f], send_sem=csend.at[f], recv_sem=crcv.at[f],
                device_id=where_is(owner(f)), device_id_type=MESH).wait_recv()

    lanes = lax.broadcasted_iota(jnp.int32, (NB, 2 * NB), 1)
    signs = jnp.where(lanes < NB, 1.0, -1.0).astype(jnp.bfloat16)
    wide_lane = lax.broadcasted_iota(jnp.int32, (1, NF), 1)
    energies = jnp.zeros((1, NF), jnp.float32)
    for f in range(NF):
        pairs = crecv[f, :16, :]
        straight = jnp.concatenate([pairs[:, : 2 * NB], pairs[:, 2 * NB :]], axis=0)
        crossed = jnp.concatenate([straight[:, NB:], straight[:, :NB]], axis=1)
        stacked = jnp.concatenate([straight * signs, crossed], axis=0)
        tiled = jnp.concatenate([stacked] * 3, axis=1)
        full = jnp.dot(spread_ref[...], tiled, preferred_element_type=jnp.float32)
        full = (full * mask_ref[...]).astype(jnp.bfloat16)
        modes_ref[f * 6 * NB : (f + 1) * 6 * NB, :] = jnp.dot(
            full, spec[f], preferred_element_type=jnp.float32).astype(jnp.bfloat16)
        tail = crecv[f, 16:, :].astype(jnp.float32)
        energies = jnp.where(wide_lane == f, jnp.sum(tail[:1, :], axis=1, keepdims=True), energies)
    energy_ref[...] = energies

    @pl.when(owns)
    def _():
        @pl.loop(1, total)
        def _(k):
            coef_to((lin + k) % total).wait_send()


def fused(n, nf_dev, chosen, snapshots, block_starts, freq_index):
    per, whole, shared, holders = chosen
    rows, count, wide = snapshots.shape
    total = n * nf_dev
    pw = wide // n
    slots = per + 4
    f32, bf16 = jnp.float32, jnp.bfloat16
    dma = pltpu.SemaphoreType.DMA
    vmem = pl.BlockSpec(memory_space=pltpu.VMEM)
    modes, energy = pl.pallas_call(
        functools.partial(kernel, n, nf_dev, per, whole, shared, holders, float(wide * nf_dev)),
        out_shape=(jax.ShapeDtypeStruct((NF * NB * 6, pw), bf16), jax.ShapeDtypeStruct((1, NF), f32)),
        in_specs=[pl.BlockSpec(memory_space=pltpu.HBM)] * 2,
        out_specs=(vmem, vmem),
        scratch_shapes=[
            pltpu.SMEM((NB + NF,), jnp.int32),
            pltpu.VMEM((slots * ROWS, rows), bf16),
            pltpu.VMEM((NB * 6, 2 * NB), bf16),
            pltpu.VMEM((NB * 6, 6 * NB), f32),
            pltpu.VMEM((3, rows, wide), bf16),
            pltpu.VMEM((slots, 2, 3, ROWS, wide // 2), f32),
            pltpu.VMEM((slots, 3, ROWS, wide // 2), f32),
            pltpu.VMEM((slots, n, ROWS, 3 * pw), bf16),
            pltpu.VMEM((NB, ROWS, 3 * pw), bf16),
            pltpu.VMEM((3, NB * ROWS, pw), f32),
            pltpu.VMEM((NF, 6 * NB, pw), bf16),
            pltpu.VMEM((NF, NB // 2, 4 * NB), f32),
            pltpu.VMEM((total, NB // 2, 4 * NB), f32),
            pltpu.VMEM((32, 4 * NB), bf16),
            pltpu.VMEM((NF, 32, 4 * NB), bf16),
            dma((4,)), dma((slots,)), dma((slots,)), dma((slots, n)), dma((NB,)),
            dma((NF,)), dma((total,)), dma((total,)), dma((NF,)),
        ],
        compiler_params=pltpu.CompilerParams(
            collective_id=0, has_side_effects=True, vmem_limit_bytes=54_000_000),
    )(jnp.transpose(snapshots, (1, 0, 2)), jnp.concatenate([block_starts, freq_index]))
    modes = modes.reshape(NF, NB, 3, 2, pw).transpose(0, 1, 3, 2, 4)
    return modes, energy.reshape(NF)


def solution(mesh):
    n, nf_dev = mesh.shape["tm"], mesh.shape["freq"]

    def body(snapshots, block_starts, freq_index):
        rows, _, wide = snapshots.shape
        chosen = plan(n, rows, n * nf_dev, wide // n)
        if chosen is None:
            return local(snapshots, block_starts, freq_index)
        return fused(n, nf_dev, chosen, snapshots, block_starts, freq_index)

    return jax.shard_map(
        body,
        mesh=mesh,
        in_specs=(P("tm", None, "freq"), P(), P()),
        out_specs=(P(None, None, None, None, ("freq", "tm")), P()),
        check_vma=False,
    )
```
